512 devices in a mesh: seq: 32 (over x_hi, y, core), doc: 16 (over x_lo, z).
Axes of the slice: x: 4 (x_hi: 2, x_lo: 2; x = x_hi * 2 + x_lo), y: 8, z: 8, core: 2. Of those that a mesh axis runs over, the one named last changes fastest.
Arguments:
- hidden: bfloat16 [16, 4096, 768], P('doc', 'seq'), may hold values from -3 to 3
- queries: bfloat16 [16, 4096, 768], P('doc', 'seq'), may hold values from -8 to 8
- key_states: bfloat16 [16, 4096, 768], P('doc', 'seq'), may hold values from -8 to 8
- values: bfloat16 [16, 4096, 768], P('doc', 'seq'), may hold values from -8 to 8
- targets: int32 [16, 4096], P('doc', 'seq'), may hold values from 0 to 26623
- lengths: int32 [16], replicated, may hold values from 2048 to 4096
- keep_rank: int32 [1], replicated, may hold values from 0 to 99
- out_weight: bfloat16 [768, 768], replicated, may hold values from -0.21875 to 0.21875
- final_gain: float32 [768], replicated, may hold values from 0.5 to 1.5
- unembed: bfloat16 [768, 26624], P(None, 'doc'), may hold values from -0.390625 to 0.390625
Outputs:
- token_nll: float32 [16, 4096], P('doc', 'seq')
- log_perplexity: float32 [16], replicated
- acceptance: float32 [16], replicated
The draws below stay inside these ranges and needn't reach their ends.
All inputs are finite; a program needn't handle non-finite values.
Results may differ from the reference program's by a relative error of at most 0.007.
Values may be sent and summed in bfloat16 or wider, within the bound.
A program may use at most 64 MiB of HBM per device.

```python
import math
import jax
import jax.numpy as jnp
import numpy as np
from jax import lax

D = 768
HEADS = 12
HEAD_DIM = 64
ROT = 16
V = 26624
LENGTH = 4096
DOCS = 16


def draw_values(key, part):
    rough_key = jax.random.fold_in(key, 11)
    drift_key = jax.random.fold_in(key, 12)
    run_count = LENGTH // 32
    drift = jax.random.normal(drift_key, (DOCS, run_count, 1, D), jnp.float32)
    drift = jnp.broadcast_to(drift, (DOCS, run_count, 32, D)).reshape(DOCS, LENGTH, D)
    rough = jax.random.normal(rough_key, (DOCS, LENGTH, D), jnp.float32)
    return jnp.clip(rough + drift, -8.0, 8.0).astype(jnp.bfloat16)


def draw_queries(key, part):
    base = jnp.clip(jax.random.normal(jax.random.fold_in(key, 21), (DOCS, LENGTH, D), jnp.float32), -6.0, 6.0)
    return base.astype(jnp.bfloat16)


def draw_key_states(key, part):
    base = jnp.clip(jax.random.normal(jax.random.fold_in(key, 22), (DOCS, LENGTH, D), jnp.float32), -6.0, 6.0)
    return base.astype(jnp.bfloat16)


def draw_hidden(key, part):
    base = jnp.clip(0.5 * jax.random.normal(jax.random.fold_in(key, 23), (DOCS, LENGTH, D), jnp.float32), -3.0, 3.0)
    return base.astype(jnp.bfloat16)


def draw_unembed(key, part):
    limit = 300.0 / D
    base = jax.random.normal(jax.random.fold_in(key, 24), (D, V), jnp.float32) / math.sqrt(D)
    return jnp.clip(base, -limit, limit).astype(jnp.bfloat16)


def touch_ends(values, own_key, low, top_value):
    longest = values.shape.index(max(values.shape))
    spots = []
    for shift in (0, 1):
        where = [jax.random.randint(jax.random.fold_in(own_key, axis), (), 0, length) for axis, length in enumerate(values.shape)]
        where[longest] = (where[longest] + shift) % values.shape[longest]
        spots.append(tuple(where))
    return values.at[spots[0]].set(low).at[spots[1]].set(top_value)


def rank_table(amount, lean):
    loads = [(1 << 20) // math.isqrt(standing ** lean) + 1 for standing in range(1, amount + 1)]
    scale = 1 + sum(loads) // (1 << 30)
    return np.cumsum(np.array([max(1, weight // scale) for weight in loads]))


def ranked(stream_key, extent, count, slope):
    grid = rank_table(count, slope)
    ticket = jax.random.randint(jax.random.fold_in(stream_key, 1), extent, 0, int(grid[count - 1]))
    rank = jnp.searchsorted(jnp.asarray(grid, jnp.int32), ticket, side="right")
    return jax.random.permutation(jax.random.fold_in(stream_key, 2), count)[rank].astype(jnp.int32)


def gaussian(rng, extent, scale, bound, kind=jnp.bfloat16):
    values = scale * jax.random.normal(rng, extent, jnp.float32)
    return jnp.clip(values, min=-bound, max=bound).astype(kind)


def setup_inputs(seed: int = 0) -> dict:
    streams_of = jax.random.split(jax.random.key(seed), 11)
    return {
        "hidden": draw_hidden(jax.random.fold_in(streams_of[10], 71), 0),
        "queries": draw_queries(jax.random.fold_in(streams_of[10], 71), 0),
        "key_states": draw_key_states(jax.random.fold_in(streams_of[10], 71), 0),
        "values": draw_values(jax.random.fold_in(streams_of[10], 71), 0),
        "targets": touch_ends(ranked(streams_of[4], (DOCS, LENGTH), V, 2), jax.random.fold_in(streams_of[4], 3), 0, V - 1).astype(jnp.int32),
        "lengths": touch_ends(jax.random.randint(streams_of[5], (DOCS,), LENGTH // 2, LENGTH + 1), jax.random.fold_in(streams_of[5], 1), LENGTH // 2, LENGTH).astype(jnp.int32),
        "keep_rank": jax.random.randint(streams_of[6], (1,), 0, 100).astype(jnp.int32),
        "out_weight": gaussian(streams_of[7], (D, D), D ** -0.5, 0.21875),
        "final_gain": jnp.clip(1.0 + 0.1 * jax.random.normal(streams_of[8], (D,), jnp.float32), 0.5, 1.5),
        "unembed": draw_unembed(jax.random.fold_in(streams_of[10], 71), 0),
    }


NEGATIVE = -1e+30
ROTARY_BASE = 10000.0
NORM_EPSILON = 1e-05
SPREAD_EPSILON = 0.0001

def round_trip(tensor):
    return lax.optimization_barrier(tensor.astype(jnp.bfloat16)).astype(jnp.float32)

def rotate(block, first_row):
    row_count = block.shape[0]
    half_rot = ROT // 2
    where_at = (first_row + jnp.arange(row_count, dtype=jnp.int32)).astype(jnp.float32)
    inv_freq = ROTARY_BASE ** (-2.0 * jnp.arange(half_rot, dtype=jnp.int32).astype(jnp.float32) / ROT)
    angles = where_at[:, None] * inv_freq[None, :]
    cosine = jnp.cos(angles)[:, None, :]
    sine_part = jnp.sin(angles)[:, None, :]
    per_head = block.reshape(row_count, HEADS, HEAD_DIM)
    low_half = per_head[:, :, :half_rot]
    high_half = per_head[:, :, half_rot:ROT]
    turned = jnp.concatenate([low_half * cosine - high_half * sine_part, high_half * cosine + low_half * sine_part, per_head[:, :, ROT:]], axis=2)
    return turned.reshape(row_count, HEADS * HEAD_DIM)

def accept(log_perplexity, keep_rank):
    doc_count = log_perplexity.shape[0]
    center = log_perplexity - jnp.mean(log_perplexity)
    spread = jnp.sqrt(jnp.mean(center * center) + SPREAD_EPSILON)
    ordered = jnp.sort(log_perplexity)
    scaled_rank = (keep_rank[0] * (doc_count - 1)).astype(jnp.int32)
    low_index = (scaled_rank // 99).astype(jnp.int32)
    high_index = jnp.minimum(low_index + 1, doc_count - 1).astype(jnp.int32)
    fraction = (scaled_rank - 99 * low_index).astype(jnp.float32) / 99.0
    places = jnp.arange(doc_count, dtype=jnp.int32)
    low_value = jnp.sum(jnp.where(places == low_index, ordered, 0.0))
    high_value = jnp.sum(jnp.where(places == high_index, ordered, 0.0))
    rank_level = (1.0 - fraction) * low_value + fraction * high_value
    return jax.nn.sigmoid((rank_level - log_perplexity) / spread)

def score_document(hidden, queries, key_states, values, targets, doc_length, out_weight, final_gain, unembed):
    turned_q = rotate(queries.astype(jnp.float32), 0)
    turned_k = rotate(key_states.astype(jnp.float32), 0)
    query_all = round_trip(turned_q)
    key_heads = round_trip(turned_k).reshape(LENGTH, HEADS, HEAD_DIM)
    value_heads = values.astype(jnp.float32).reshape(LENGTH, HEADS, HEAD_DIM)
    block_rows = math.gcd(512, LENGTH)
    score_scale = 1.0 / math.sqrt(HEAD_DIM)
    key_place = jnp.arange(LENGTH, dtype=jnp.int32)

    def attend(block_index):
        begin_at = block_index * block_rows
        query_heads = lax.dynamic_slice_in_dim(query_all, begin_at, block_rows, 0).reshape(block_rows, HEADS, HEAD_DIM)
        scores = jnp.einsum('qhd,khd->hqk', query_heads, key_heads) * score_scale
        query_place = begin_at + jnp.arange(block_rows, dtype=jnp.int32)
        allowed = key_place[None, None, :] <= query_place[None, :, None]
        scores = jnp.where(allowed, scores, NEGATIVE)
        top_score = lax.optimization_barrier(jnp.max(scores, axis=2, keepdims=True))
        weights = jnp.where(allowed, jnp.exp(scores - top_score), 0.0)
        totals = lax.optimization_barrier(jnp.sum(weights, axis=2))
        summed = jnp.einsum('hqk,khd->qhd', round_trip(weights), value_heads)
        return (summed / jnp.transpose(totals)[:, :, None]).reshape(block_rows, HEADS * HEAD_DIM).astype(jnp.bfloat16)
    attended = lax.map(attend, jnp.arange(LENGTH // block_rows, dtype=jnp.int32)).reshape(LENGTH, HEADS * HEAD_DIM)
    residual = hidden.astype(jnp.float32) + jnp.dot(attended, out_weight, preferred_element_type=jnp.float32)
    center = residual - lax.optimization_barrier(jnp.mean(residual, axis=1, keepdims=True))
    spread = lax.optimization_barrier(jnp.mean(center * center, axis=1, keepdims=True))
    normed = (center * lax.rsqrt(spread + NORM_EPSILON) * final_gain).astype(jnp.bfloat16)

    def shard_stats(block_index):
        begin_at = block_index * block_rows
        block = lax.dynamic_slice_in_dim(normed, begin_at, block_rows, 0)
        logits = jnp.dot(block, unembed, preferred_element_type=jnp.float32)
        top_score = lax.optimization_barrier(jnp.max(logits, axis=1))
        totals = lax.optimization_barrier(jnp.sum(jnp.exp(logits - top_score[:, None]), axis=1))
        wanted = lax.dynamic_slice_in_dim(targets, begin_at, block_rows, 0)
        matches = jnp.arange(V, dtype=jnp.int32)[None, :] == wanted[:, None]
        picked = lax.optimization_barrier(jnp.sum(jnp.where(matches, logits, 0.0), axis=1))
        return top_score + jnp.log(totals) - picked
    token_loss = lax.map(shard_stats, jnp.arange(LENGTH // block_rows, dtype=jnp.int32)).reshape(LENGTH)
    is_valid = jnp.arange(LENGTH, dtype=jnp.int32) < doc_length
    token_loss = jnp.where(is_valid, token_loss, 0.0)
    return (token_loss, jnp.sum(token_loss) / doc_length.astype(jnp.float32))

def reference(hidden, queries, key_states, values, targets, lengths, keep_rank, out_weight, final_gain, unembed):

    def per_document(bundle):
        return score_document(bundle[0], bundle[1], bundle[2], bundle[3], bundle[4], bundle[5], out_weight, final_gain, unembed)
    token_nll, log_perplexity = lax.map(per_document, (hidden, queries, key_states, values, targets, lengths))
    acceptance = accept(log_perplexity, keep_rank)
    return (token_nll, log_perplexity, acceptance)
```

```python
import math

import jax
import jax.numpy as jnp
from jax import lax
from jax.experimental import pallas as pl
from jax.experimental.pallas import tpu as pltpu
from jax.sharding import Mesh
from jax.sharding import PartitionSpec as P

HEADS = 12
HEAD_DIM = 64
ROT = 16
D = 768
ROWS = 128
SHARE = 1664
WIDE = 2 * SHARE
TILE = 256
TILES = WIDE // TILE
DOCS = 16
SEQ = 32
CHUNK = 512
NEGATIVE = -1e30
ROTARY_BASE = 10000.0
NORM_EPSILON = 1e-05
SPREAD_EPSILON = 0.0001
LOG2E = 1.4426950408889634
MESH = pl.DeviceIdType.MESH
F32 = jnp.float32
BF16 = jnp.bfloat16


def lanes(shape):
    return lax.broadcasted_iota(jnp.int32, shape, len(shape) - 1)


def rows_of(shape):
    return lax.broadcasted_iota(jnp.int32, shape, len(shape) - 2)


def rcopy(src, dst, ss, rs, **where):
    return pltpu.make_async_remote_copy(
        src_ref=src,
        dst_ref=dst,
        send_sem=ss,
        recv_sem=rs,
        device_id=where,
        device_id_type=MESH,
    )


def kernel(
    lengths_ref,
    rank_ref,
    q_ref,
    k_ref,
    v_ref,
    hid_ref,
    cos_ref,
    sin_ref,
    tgt_ref,
    gain_ref,
    ow_ref,
    un_ref,
    nll_ref,
    ppl_ref,
    acc_out_ref,
    packed,
    got,
    outs,
    att,
    attended,
    qt,
    s_scr,
    mx_ref,
    sum_ref,
    pv_ref,
    wide,
    rows_buf,
    relay,
    logit,
    tgts,
    stat_out,
    stats,
    seqs,
    docs,
    a_send,
    a_recv,
    f_send,
    f_recv,
    r_send,
    r_recv,
    w_sem,
    c_send,
    c_recv,
    t_send,
    t_recv,
    s_send,
    s_recv,
    q_send,
    q_recv,
    d_send,
    d_recv,
):
    xh = lax.axis_index("xh")
    y = lax.axis_index("y")
    c = lax.axis_index("c")
    xl = lax.axis_index("xl")
    z = lax.axis_index("z")
    me = xh * 8 + y
    seq = me * 2 + c
    doc = xl * 8 + z
    sig = 1 - 2 * lax.rem(z, 2)
    z_up = lax.rem(z + sig + 8, 8)
    z_dn = lax.rem(z - sig + 8, 8)
    z_pair = z + sig

    barrier = pltpu.get_barrier_semaphore()

    def greet_seq(n, carry):
        @pl.when(n != seq)
        def _():
            pl.semaphore_signal(
                barrier,
                inc=1,
                device_id={"xh": n // 16, "y": lax.rem(n // 2, 8), "c": lax.rem(n, 2)},
                device_id_type=MESH,
            )

        return carry

    def greet_doc(n, carry):
        @pl.when(n != doc)
        def _():
            pl.semaphore_signal(
                barrier,
                inc=1,
                device_id={"xl": n // 8, "z": lax.rem(n, 8)},
                device_id_type=MESH,
            )

        return carry

    lax.fori_loop(0, SEQ, greet_seq, 0)
    lax.fori_loop(0, DOCS, greet_doc, 0)

    mine = pltpu.make_async_copy(un_ref, wide.at[:, pl.ds(0, SHARE)], w_sem.at[4])
    mine.start()

    lane = lanes((ROWS, ROWS))
    low = lane < HEAD_DIM
    first = lax.rem(lane, HEAD_DIM) < ROT // 2
    cosine = cos_ref[...]
    sine = sin_ref[...]
    low_half = low[:HEAD_DIM]

    def turn(block):
        partner = jnp.where(first, pltpu.roll(block, ROWS - 8, 1), pltpu.roll(block, 8, 1))
        return block * cosine + partner * sine

    for pair in range(HEADS // 2):
        at = slice(pair * ROWS, (pair + 1) * ROWS)
        tk = turn(k_ref[:, at].astype(F32))
        tq = turn(q_ref[:, at].astype(F32))
        tv = v_ref[:, at].astype(F32)
        rk = pltpu.roll(tk, HEAD_DIM, 1)
        rq = pltpu.roll(tq, HEAD_DIM, 1)
        rv = pltpu.roll(tv, HEAD_DIM, 1)
        packed[2 * pair, 0:ROWS] = jnp.where(low, tk, rv).astype(BF16)
        packed[2 * pair + 1, 0:ROWS] = jnp.where(low, rk, tv).astype(BF16)
        packed[2 * pair, ROWS : ROWS + HEAD_DIM] = jnp.where(
            low_half, tq[:HEAD_DIM], rq[HEAD_DIM:]
        ).astype(BF16)
        packed[2 * pair + 1, ROWS : ROWS + HEAD_DIM] = jnp.where(
            low_half, rq[:HEAD_DIM], tq[HEAD_DIM:]
        ).astype(BF16)

    pl.semaphore_wait(barrier, SEQ - 1 + DOCS - 1)

    is_head = jnp.logical_and(y != 3, y != 7)
    my_slot = y - jnp.where(y > 3, 1, 0)
    my_head = jnp.where(is_head, xh * 6 + my_slot, -1)

    def head_copy(h):
        yi = lax.rem(h, 6)
        return rcopy(
            packed.at[h],
            got.at[seq],
            a_send.at[h],
            a_recv.at[me],
            xh=h // 6,
            y=yi + jnp.where(yi > 2, 1, 0),
        )

    def send_head(n, carry):
        h = lax.rem(n + me, HEADS)

        @pl.when(h != my_head)
        def _():
            head_copy(h).start()

        @pl.when(h == my_head)
        def _():
            got[seq] = packed[h]

        return carry

    lax.fori_loop(0, HEADS, send_head, 0)

    half_rows = pl.ds(pl.multiple_of(c * (D // 2), D // 2), D // 2)
    swap = rcopy(
        un_ref.at[half_rows],
        wide.at[half_rows, pl.ds(SHARE, SHARE)],
        w_sem.at[0],
        w_sem.at[1],
        z=z_pair,
    )
    swap.start()

    def target_copy(n):
        side = n // 4
        step = lax.rem(n, 4)
        move = jnp.where(
            step == 0, 0, jnp.where(step == 1, -sig, jnp.where(step == 2, 2 * sig, -3 * sig))
        )
        return rcopy(
            tgt_ref,
            tgts.at[n],
            t_send.at[n],
            t_recv.at[n],
            xl=lax.rem(xl + side, 2),
            z=lax.rem(z + move + 8, 8),
        )

    tgts[0] = tgt_ref[...]

    def send_target(n, carry):
        target_copy(n).start()
        return carry

    lax.fori_loop(1, 8, send_target, 0)

    def arrival(i):
        @pl.when(i != me)
        def _():
            rcopy(
                packed.at[0], got.at[2 * i + c], a_send.at[0], a_recv.at[i], xh=xh, y=y
            ).wait_recv()

        forward(i).start()

    def forward(i):
        piece = got.at[2 * i + c, pl.ds(0, ROWS)]
        return rcopy(piece, piece, f_send.at[i], f_recv.at[i], c=1 - c)

    def forwarded(i):
        piece = got.at[2 * i + 1 - c, pl.ds(0, ROWS)]
        return rcopy(piece, piece, f_send.at[i], f_recv.at[i], c=1 - c)

    scale = LOG2E / math.sqrt(HEAD_DIM)

    def result_copy(i):
        return rcopy(
            outs.at[i],
            att.at[my_head],
            r_send.at[i],
            r_recv.at[my_head],
            xh=i // 8,
            y=lax.rem(i, 8),
        )

    def query_step(t, carry):
        @pl.when(t < 7)
        def _():
            arrival(2 * t + 2)
            arrival(2 * t + 3)

        for u in range(2):
            qp = got[4 * t + 2 * u + c, ROWS : ROWS + HEAD_DIM].astype(F32)
            qt[u * ROWS : u * ROWS + HEAD_DIM] = jnp.where(low_half, qp, 0.0).astype(BF16)
            qt[u * ROWS + HEAD_DIM : (u + 1) * ROWS] = jnp.where(
                low_half, pltpu.roll(qp, HEAD_DIM, 1), 0.0
            ).astype(BF16)
        mx_ref[...] = jnp.full((2 * ROWS, ROWS), NEGATIVE, F32)
        sum_ref[...] = jnp.zeros((2 * ROWS, ROWS), F32)
        pv_ref[...] = jnp.zeros((2 * ROWS, ROWS), F32)
        forwarded(2 * t).wait_recv()
        forwarded(2 * t + 1).wait_recv()

        def scores(j, masked):
            block = got[pl.ds(4 * j, 4), 0:ROWS].reshape(CHUNK, ROWS)
            s = lax.dot_general(
                qt[...], block, (((1,), (1,)), ((), ())), preferred_element_type=F32
            )
            if masked:
                shape = (2 * ROWS, CHUNK)
                row = rows_of(shape)
                place = row + jnp.where(row >= ROWS, ROWS, 0) + c * ROWS
                s = jnp.where(lanes(shape) <= place, s, NEGATIVE)
            s_scr[j] = s
            top = mx_ref[...]
            for g in range(CHUNK // ROWS):
                top = jnp.maximum(top, s[:, g * ROWS : (g + 1) * ROWS])
            mx_ref[...] = top

        def plain(j, inner):
            scores(j, False)
            return inner

        lax.fori_loop(0, t, plain, 0)
        scores(t, True)
        top = jnp.max(mx_ref[...], axis=1, keepdims=True) * scale

        def weigh(j, inner):
            block = got[pl.ds(4 * j, 4), 0:ROWS].reshape(CHUNK, ROWS)
            p = jnp.exp2(s_scr[j] * scale - top)
            total = sum_ref[...]
            for g in range(CHUNK // ROWS):
                total = total + p[:, g * ROWS : (g + 1) * ROWS]
            sum_ref[...] = total
            pv_ref[...] += jnp.dot(p.astype(BF16), block, preferred_element_type=F32)
            return inner

        lax.fori_loop(0, t + 1, weigh, 0)
        out = pv_ref[...] / jnp.sum(sum_ref[...], axis=1, keepdims=True)
        for u in range(2):
            i = 2 * t + u
            top_part = out[u * ROWS : u * ROWS + HEAD_DIM]
            bottom = out[u * ROWS + HEAD_DIM : (u + 1) * ROWS]
            whole = jnp.where(low_half, pltpu.roll(top_part, HEAD_DIM, 1), bottom).astype(BF16)
            outs[i] = whole

            @pl.when(i != me)
            def _():
                result_copy(i).start()

            @pl.when(i == me)
            def _():
                att[my_head] = whole

        return carry

    @pl.when(is_head)
    def _():
        arrival(0)
        arrival(1)
        lax.fori_loop(0, 8, query_step, 0)

    swap.wait_recv()
    share = wide.at[half_rows, pl.ds(SHARE, SHARE)]
    pass_on = rcopy(share, share, w_sem.at[2], w_sem.at[3], c=1 - c)
    pass_on.start()

    def wait_result(h, carry):
        @pl.when(h != my_head)
        def _():
            rcopy(outs.at[0], att.at[h], r_send.at[0], r_recv.at[h], xh=xh, y=y).wait_recv()

        return carry

    lax.fori_loop(0, HEADS, wait_result, 0)
    for pair in range(HEADS // 2):
        at = slice(pair * ROWS, (pair + 1) * ROWS)
        even = att[2 * pair].astype(F32)
        odd = att[2 * pair + 1].astype(F32)
        attended[0:HEAD_DIM, at] = jnp.where(
            low_half, even, pltpu.roll(odd, HEAD_DIM, 1)
        ).astype(BF16)
        attended[HEAD_DIM:ROWS, at] = jnp.where(
            low_half, pltpu.roll(even, HEAD_DIM, 1), odd
        ).astype(BF16)
    residual = hid_ref[...].astype(F32) + jnp.dot(
        attended[...], ow_ref[...], preferred_element_type=F32
    )
    center = residual - jnp.sum(residual, axis=1, keepdims=True) * (1.0 / D)
    spread = jnp.sum(center * center, axis=1, keepdims=True) * (1.0 / D)
    rows_buf[0] = (center * lax.rsqrt(spread + NORM_EPSILON) * gain_ref[...]).astype(BF16)

    def row_copy(n):
        if n < 4:
            return rcopy(
                rows_buf.at[n], rows_buf.at[4 + n], c_send.at[n], c_recv.at[4 + n], xl=1 - xl
            )
        if n == 4:
            return rcopy(rows_buf.at[0], rows_buf.at[1], c_send.at[4], c_recv.at[1], z=z_dn)
        if n == 5:
            return rcopy(rows_buf.at[0], relay.at[0], c_send.at[5], c_recv.at[8], z=z_up)
        if n == 6:
            return rcopy(rows_buf.at[1], relay.at[1], c_send.at[6], c_recv.at[9], z=z_up)
        if n == 7:
            return rcopy(relay.at[0], rows_buf.at[2], c_send.at[7], c_recv.at[2], z=z_dn)
        return rcopy(relay.at[1], rows_buf.at[3], c_send.at[8], c_recv.at[3], z=z_dn)

    def row_wait(slot):
        ref = relay.at[slot - 8] if slot >= 8 else rows_buf.at[slot]
        rcopy(rows_buf.at[0], ref, c_send.at[0], c_recv.at[slot], z=z_dn).wait_recv()

    row_copy(4).start()
    row_copy(5).start()
    row_copy(0).start()
    mine.wait()
    pass_on.wait_recv()

    def wait_target(n, carry):
        rcopy(tgt_ref, tgts.at[n], t_send.at[n], t_recv.at[n], z=z_dn).wait_recv()
        return carry

    lax.fori_loop(1, 8, wait_target, 0)
    diagonal = lane == rows_of((ROWS, ROWS))
    other = xl * 8 + z_pair

    def stat_copy(slot):
        side = slot // 4
        back = lax.rem(z - sig * lax.rem(slot, 4) + 8, 8)
        return rcopy(
            stat_out.at[slot],
            stats.at[xl * 4 + z // 2],
            s_send.at[slot],
            s_recv.at[xl * 4 + z // 2],
            xl=lax.rem(xl + side, 2),
            z=back,
        )

    def as_row(column):
        return jnp.sum(jnp.where(diagonal, column, 0.0), axis=0, keepdims=True)

    def score_rows(n, carry):
        slot = lax.rem(n, 2) * 4 + n // 2

        @pl.when(n == 1)
        def _():
            row_wait(1)
            row_copy(6).start()
            row_copy(1).start()
            row_wait(8)
            row_copy(7).start()
            row_wait(4)

        @pl.when(n == 2)
        def _():
            row_wait(9)
            row_copy(8).start()
            row_wait(2)
            row_copy(2).start()

        @pl.when(n == 3)
        def _():
            row_wait(5)

        @pl.when(n == 4)
        def _():
            row_wait(3)
            row_copy(3).start()

        @pl.when(n == 5)
        def _():
            row_wait(6)

        @pl.when(n == 7)
        def _():
            row_wait(7)

        block = rows_buf[slot]
        mx_ref[0:ROWS] = jnp.full((ROWS, ROWS), NEGATIVE, F32)

        def multiply(k, inner):
            s = jnp.dot(
                block,
                wide[:, pl.ds(pl.multiple_of(k * TILE, TILE), TILE)],
                preferred_element_type=F32,
            )
            logit[k] = s
            mx_ref[0:ROWS] = jnp.maximum(
                mx_ref[0:ROWS], jnp.maximum(s[:, :ROWS], s[:, ROWS:])
            )
            return inner

        lax.fori_loop(0, TILES, multiply, 0)
        wanted = jnp.sum(jnp.where(diagonal, tgts[slot], 0.0), axis=1, keepdims=True)
        wanted = wanted.astype(jnp.int32)
        here = wanted - doc * SHARE
        there = wanted - other * SHARE
        place = jnp.where(
            jnp.logical_and(here >= 0, here < SHARE),
            here,
            jnp.where(jnp.logical_and(there >= 0, there < SHARE), there + SHARE, -1),
        )
        place = jnp.broadcast_to(place, (ROWS, ROWS)) - lane
        top = jnp.max(mx_ref[0:ROWS], axis=1, keepdims=True)
        top2 = jnp.broadcast_to(top * LOG2E, (ROWS, ROWS))
        sum_ref[0:ROWS] = jnp.zeros((ROWS, ROWS), F32)
        pv_ref[0:ROWS] = jnp.zeros((ROWS, ROWS), F32)

        def add_up(k, inner):
            total = sum_ref[0:ROWS]
            pick = pv_ref[0:ROWS]
            for g in range(TILE // ROWS):
                s = logit[k, :, g * ROWS : (g + 1) * ROWS]
                total = total + jnp.exp2(s * LOG2E - top2)
                pick = pick + jnp.where(place == k * TILE + g * ROWS, s, 0.0)
            sum_ref[0:ROWS] = total
            pv_ref[0:ROWS] = pick
            return inner

        lax.fori_loop(0, TILES, add_up, 0)
        lse = top + jnp.log(jnp.sum(sum_ref[0:ROWS], axis=1, keepdims=True))
        pick = jnp.sum(pv_ref[0:ROWS], axis=1, keepdims=True)
        row8 = rows_of((8, ROWS))
        tile = jnp.where(row8 == 0, as_row(lse), as_row(pick))

        @pl.when(n != 0)
        def _():
            stat_out[slot] = tile
            stat_copy(slot).start()

        @pl.when(n == 0)
        def _():
            stats[xl * 4 + z // 2] = tile

        return carry

    lax.fori_loop(0, 8, score_rows, 0)

    def wait_stat(n, carry):
        @pl.when(n != xl * 4 + z // 2)
        def _():
            rcopy(stat_out.at[0], stats.at[n], s_send.at[0], s_recv.at[n], z=z_dn).wait_recv()

        return carry

    lax.fori_loop(0, 8, wait_stat, 0)
    parts = [stats[n] for n in range(8)]
    top = parts[0][0:1]
    for part in parts[1:]:
        top = jnp.maximum(top, part[0:1])
    total = jnp.zeros((1, ROWS), F32)
    pick = jnp.zeros((1, ROWS), F32)
    for part in parts:
        total = total + jnp.exp(part[0:1] - top)
        pick = pick + part[1:2]
    place = seq * ROWS + lanes((1, ROWS))
    nll = jnp.where(place < lengths_ref[doc], top + jnp.log(total) - pick, 0.0)
    nll_ref[...] = nll
    seqs[seq] = jnp.broadcast_to(jnp.sum(nll, axis=1, keepdims=True), (1, ROWS))

    def seq_copy(n):
        return rcopy(
            seqs.at[seq],
            seqs.at[seq],
            q_send.at[n],
            q_recv.at[seq],
            xh=n // 16,
            y=lax.rem(n // 2, 8),
            c=lax.rem(n, 2),
        )

    def send_seq(n, carry):
        @pl.when(n != seq)
        def _():
            seq_copy(n).start()

        return carry

    def wait_seq(n, carry):
        @pl.when(n != seq)
        def _():
            rcopy(seqs.at[n], seqs.at[n], q_send.at[n], q_recv.at[n], xh=xh, y=y, c=c).wait_recv()

        return carry

    lax.fori_loop(0, SEQ, send_seq, 0)
    lax.fori_loop(0, SEQ, wait_seq, 0)
    docs[doc] = jnp.sum(seqs[...], axis=0)

    def doc_copy(n):
        return rcopy(
            docs.at[doc],
            docs.at[doc],
            d_send.at[n],
            d_recv.at[doc],
            xl=n // 8,
            z=lax.rem(n, 8),
        )

    def send_doc(n, carry):
        @pl.when(n != doc)
        def _():
            doc_copy(n).start()

        return carry

    def wait_doc(n, carry):
        @pl.when(n != doc)
        def _():
            rcopy(docs.at[n], docs.at[n], d_send.at[n], d_recv.at[n], xl=xl, z=z).wait_recv()

        return carry

    lax.fori_loop(0, DOCS, send_doc, 0)
    lax.fori_loop(0, DOCS, wait_doc, 0)

    shape = (DOCS, ROWS)
    row = rows_of(shape)
    col = lanes(shape)
    column = docs[...].reshape(DOCS, ROWS)
    for d in range(DOCS):
        column = jnp.where(row == d, column / lengths_ref[d].astype(F32), column)
    valid = lanes((1, ROWS)) < DOCS
    line = jnp.sum(jnp.where(row == col, column, 0.0), axis=0, keepdims=True)
    mean = jnp.sum(line, axis=1, keepdims=True) * (1.0 / DOCS)
    off = jnp.where(valid, line - mean, 0.0)
    spread = jnp.sqrt(jnp.sum(off * off, axis=1, keepdims=True) * (1.0 / DOCS) + SPREAD_EPSILON)
    ahead = jnp.logical_or(
        column < line, jnp.logical_and(column == line, row < col)
    )
    rank = jnp.sum(jnp.where(ahead, 1.0, 0.0), axis=0, keepdims=True)
    scaled = rank_ref[0] * (DOCS - 1)
    low_index = lax.div(scaled, 99)
    high_index = jnp.minimum(low_index + 1, DOCS - 1)
    fraction = (scaled - 99 * low_index).astype(F32) / 99.0
    hit_low = jnp.logical_and(valid, rank == low_index.astype(F32))
    hit_high = jnp.logical_and(valid, rank == high_index.astype(F32))
    low_value = jnp.sum(jnp.where(hit_low, line, 0.0), axis=1, keepdims=True)
    high_value = jnp.sum(jnp.where(hit_high, line, 0.0), axis=1, keepdims=True)
    level = (1.0 - fraction) * low_value + fraction * high_value
    ppl_ref[...] = line
    acc_out_ref[...] = jax.nn.sigmoid((level - line) / spread)

    def drain_head(h, carry):
        @pl.when(h != my_head)
        def _():
            head_copy(h).wait_send()

        return carry

    lax.fori_loop(0, HEADS, drain_head, 0)

    def drain_work(i, carry):
        forward(i).wait_send()

        @pl.when(i != me)
        def _():
            result_copy(i).wait_send()

        return carry

    @pl.when(is_head)
    def _():
        lax.fori_loop(0, 16, drain_work, 0)

    swap.wait_send()
    pass_on.wait_send()
    for n in range(9):
        row_copy(n).wait_send()

    def drain_small(n, carry):
        target_copy(n).wait_send()
        stat_copy(n).wait_send()
        return carry

    lax.fori_loop(1, 8, drain_small, 0)

    def drain_seq(n, carry):
        @pl.when(n != seq)
        def _():
            seq_copy(n).wait_send()

        return carry

    def drain_doc(n, carry):
        @pl.when(n != doc)
        def _():
            doc_copy(n).wait_send()

        return carry

    lax.fori_loop(0, SEQ, drain_seq, 0)
    lax.fori_loop(0, DOCS, drain_doc, 0)


def shards(
    hidden,
    queries,
    key_states,
    values,
    targets,
    lengths,
    keep_rank,
    out_weight,
    final_gain,
    unembed,
):
    seq = lax.axis_index("xh") * 16 + lax.axis_index("y") * 2 + lax.axis_index("c")
    place = (seq * ROWS + jnp.arange(ROWS, dtype=jnp.int32)).astype(F32)
    spot = jnp.arange(ROWS, dtype=jnp.int32) % HEAD_DIM
    turn = (spot % (ROT // 2)).astype(F32)
    inv_freq = ROTARY_BASE ** (-2.0 * turn / ROT)
    angles = place[:, None] * inv_freq[None, :]
    cosine = jnp.where(spot < ROT, jnp.cos(angles), 1.0)
    sine = jnp.sin(angles)
    sine = jnp.where(spot < ROT // 2, -sine, jnp.where(spot < ROT, sine, 0.0))
    vmem = pl.BlockSpec(memory_space=pltpu.VMEM)
    smem = pl.BlockSpec(memory_space=pltpu.SMEM)
    dma = pltpu.SemaphoreType.DMA
    nll, ppl, acceptance = pl.pallas_call(
        kernel,
        name="scoring",
        out_shape=(
            jax.ShapeDtypeStruct((1, ROWS), F32),
            jax.ShapeDtypeStruct((1, ROWS), F32),
            jax.ShapeDtypeStruct((1, ROWS), F32),
        ),
        in_specs=[smem, smem] + [vmem] * 9 + [pl.BlockSpec(memory_space=pl.ANY)],
        out_specs=(vmem, vmem, vmem),
        scratch_shapes=[
            pltpu.VMEM((HEADS, ROWS + HEAD_DIM, ROWS), BF16),
            pltpu.VMEM((SEQ, ROWS + HEAD_DIM, ROWS), BF16),
            pltpu.VMEM((16, HEAD_DIM, ROWS), BF16),
            pltpu.VMEM((HEADS, HEAD_DIM, ROWS), BF16),
            pltpu.VMEM((ROWS, D), BF16),
            pltpu.VMEM((2 * ROWS, ROWS), BF16),
            pltpu.VMEM((8, 2 * ROWS, CHUNK), F32),
            pltpu.VMEM((2 * ROWS, ROWS), F32),
            pltpu.VMEM((2 * ROWS, ROWS), F32),
            pltpu.VMEM((2 * ROWS, ROWS), F32),
            pltpu.VMEM((D, WIDE), BF16),
            pltpu.VMEM((8, ROWS, D), BF16),
            pltpu.VMEM((2, ROWS, D), BF16),
            pltpu.VMEM((TILES, ROWS, TILE), F32),
            pltpu.VMEM((8, 1, ROWS), F32),
            pltpu.VMEM((8, 8, ROWS), F32),
            pltpu.VMEM((8, 8, ROWS), F32),
            pltpu.VMEM((SEQ, 1, ROWS), F32),
            pltpu.VMEM((DOCS, 1, ROWS), F32),
            dma((HEADS,)),
            dma((16,)),
            dma((16,)),
            dma((16,)),
            dma((16,)),
            dma((HEADS,)),
            dma((5,)),
            dma((9,)),
            dma((10,)),
            dma((8,)),
            dma((8,)),
            dma((8,)),
            dma((8,)),
            dma((SEQ,)),
            dma((SEQ,)),
            dma((DOCS,)),
            dma((DOCS,)),
        ],
        compiler_params=pltpu.CompilerParams(
            collective_id=0, has_side_effects=True, vmem_limit_bytes=48 * 1024 * 1024
        ),
    )(
        lengths,
        keep_rank,
        queries[0],
        key_states[0],
        values[0],
        hidden[0],
        cosine,
        sine,
        targets.astype(F32),
        final_gain[None, :],
        out_weight,
        unembed,
    )
    return (nll, ppl[0, :DOCS], acceptance[0, :DOCS])


def solution(mesh):
    split = Mesh(mesh.devices.reshape(2, 8, 2, 2, 8), ("xh", "y", "c", "xl", "z"))
    rows = ("xh", "y", "c")
    parts = ("xl", "z")
    placed = (
        P(parts, rows, None),
        P(parts, rows, None),
        P(parts, rows, None),
        P(parts, rows, None),
        P(parts, rows),
        P(),
        P(),
        P(),
        P(),
        P(None, parts),
    )
    return jax.shard_map(
        shards, mesh=split, in_specs=placed, out_specs=(P(parts, rows), P(), P()), check_vma=False
    )
```

```python
import math

import jax
import jax.numpy as jnp
import numpy as np
from jax import lax
from jax.experimental import pallas as pl
from jax.experimental.pallas import tpu as pltpu
from jax.sharding import Mesh
from jax.sharding import PartitionSpec as P

HEADS = 12
HEAD_DIM = 64
ROT = 16
D = 768
ROWS = 128
SHARE = 1664
WIDE = 2 * SHARE
TILE = 256
TILES = WIDE // TILE
DOCS = 16
SEQ = 32
CHUNK = 1024
SPAN = 512
NEGATIVE = -1e30
ROTARY_BASE = 10000.0
NORM_EPSILON = 1e-05
SPREAD_EPSILON = 0.0001
LOG2E = 1.4426950408889634
MESH = pl.DeviceIdType.MESH
F32 = jnp.float32
BF16 = jnp.bfloat16


def lanes(shape):
    return lax.broadcasted_iota(jnp.int32, shape, len(shape) - 1)


def rows_of(shape):
    return lax.broadcasted_iota(jnp.int32, shape, len(shape) - 2)


def rcopy(src, dst, ss, rs, **where):
    return pltpu.make_async_remote_copy(
        src_ref=src,
        dst_ref=dst,
        send_sem=ss,
        recv_sem=rs,
        device_id=where,
        device_id_type=MESH,
    )


def kernel(
    base_in,
    step_in,
    lengths_in,
    rank_in,
    q_in,
    k_in,
    v_in,
    hid_in,
    tgt_ref,
    gain_in,
    ow_in,
    un_ref,
    final_ref,
    base_ref,
    step_ref,
    lengths_ref,
    rank_ref,
    q_ref,
    k_ref,
    v_ref,
    hid_ref,
    gain_ref,
    ow_ref,
    packed,
    got,
    outs,
    att,
    attended,
    qt,
    s_scr,
    mx_ref,
    sum_ref,
    pv_ref,
    wide,
    rows_buf,
    relay,
    logit,
    tgts,
    stat_out,
    stats,
    seqs,
    docs,
    a_send,
    a_recv,
    f_send,
    f_recv,
    r_send,
    r_recv,
    w_sem,
    c_send,
    c_recv,
    t_send,
    t_recv,
    s_send,
    s_recv,
    q_send,
    q_recv,
    d_send,
    d_recv,
    i_sem,
):
    xh = lax.axis_index("xh")
    y = lax.axis_index("y")
    c = lax.axis_index("c")
    xl = lax.axis_index("xl")
    z = lax.axis_index("z")
    me = xh * 8 + y
    seq = me * 2 + c
    doc = xl * 8 + z
    sig = 1 - 2 * lax.rem(z, 2)
    z_up = lax.rem(z + sig + 8, 8)
    z_dn = lax.rem(z - sig + 8, 8)
    z_pair = z + sig

    fetches = [
        pltpu.make_async_copy(src, dst, i_sem.at[n])
        for n, (src, dst) in enumerate(
            (
                (base_in.at[lax.axis_index("xh") * 16 + lax.axis_index("y") * 2 + lax.axis_index("c")], base_ref),
                (step_in, step_ref),
                (k_in, k_ref),
                (q_in, q_ref),
                (v_in, v_ref),
                (hid_in, hid_ref),
                (ow_in, ow_ref),
                (gain_in, gain_ref),
                (lengths_in, lengths_ref),
                (rank_in, rank_ref),
                (tgt_ref, tgts.at[0]),
            )
        )
    ]
    for fetch in fetches:
        fetch.start()
    barrier = pltpu.get_barrier_semaphore()

    def peer_seq(k):
        n = lax.rem(seq + k, SEQ)
        return {"xh": lax.div(n, 16), "y": lax.rem(lax.div(n, 2), 8), "c": lax.rem(n, 2)}

    def peer_doc(k):
        n = lax.rem(doc + k, DOCS)
        return {"xl": lax.div(n, 8), "z": lax.rem(n, 8)}

    for k in range(1, SEQ):
        pl.semaphore_signal(barrier, inc=1, device_id=peer_seq(k), device_id_type=MESH)
    for k in range(1, DOCS):
        pl.semaphore_signal(barrier, inc=1, device_id=peer_doc(k), device_id_type=MESH)

    mine = pltpu.make_async_copy(un_ref, wide.at[:, pl.ds(0, SHARE)], w_sem.at[4])
    mine.start()

    lane = lanes((ROWS, ROWS))
    low = lane < HEAD_DIM
    first = lax.rem(lane, HEAD_DIM) < ROT // 2
    low_half = low[:HEAD_DIM]

    for fetch in fetches[:5]:
        fetch.wait()

    base_cos = base_ref[0:1]
    base_sin = base_ref[1:2]
    cosine = base_cos * step_ref[0] - base_sin * step_ref[1]
    sine = base_sin * step_ref[0] + base_cos * step_ref[1]
    sine = jnp.where(first, -sine, sine)

    def turn(block):
        partner = jnp.where(first, pltpu.roll(block, ROWS - 8, 1), pltpu.roll(block, 8, 1))
        return block * cosine + partner * sine

    for pair in range(HEADS // 2):
        at = slice(pair * ROWS, (pair + 1) * ROWS)
        tk = turn(k_ref[:, at].astype(F32))
        tq = turn(q_ref[:, at].astype(F32))
        tv = v_ref[:, at].astype(F32)
        rk = pltpu.roll(tk, HEAD_DIM, 1)
        rq = pltpu.roll(tq, HEAD_DIM, 1)
        rv = pltpu.roll(tv, HEAD_DIM, 1)
        packed[2 * pair, 0:ROWS] = jnp.where(low, tk, rv).astype(BF16)
        packed[2 * pair + 1, 0:ROWS] = jnp.where(low, rk, tv).astype(BF16)
        packed[2 * pair, ROWS : ROWS + HEAD_DIM] = jnp.where(
            low_half, tq[:HEAD_DIM], rq[HEAD_DIM:]
        ).astype(BF16)
        packed[2 * pair + 1, ROWS : ROWS + HEAD_DIM] = jnp.where(
            low_half, rq[:HEAD_DIM], tq[HEAD_DIM:]
        ).astype(BF16)

    pl.semaphore_wait(barrier, SEQ - 1 + DOCS - 1)

    half_rows = pl.ds(pl.multiple_of(c * (D // 2), D // 2), D // 2)
    swap = rcopy(
        un_ref.at[half_rows],
        wide.at[half_rows, pl.ds(SHARE, SHARE)],
        w_sem.at[0],
        w_sem.at[1],
        z=z_pair,
    )
    swap.start()

    is_head = jnp.logical_and(y != 3, y != 7)
    my_slot = y - jnp.where(y > 3, 1, 0)
    my_head = jnp.where(is_head, xh * 6 + my_slot, -1)

    start = lax.rem(my_head, 4)
    my_group = lax.div(me, 4)

    def head_copy(h):
        yi = lax.rem(h, 6)
        return rcopy(
            packed.at[h],
            got.at[c, me],
            a_send.at[0],
            a_recv.at[my_group],
            xh=h // 6,
            y=yi + jnp.where(yi > 2, 1, 0),
        )

    def send_head(n, carry):
        h = 4 * lax.rem(n + me, 3) + lax.rem(my_group + 4 - n // 3, 4)

        @pl.when(h != my_head)
        def _():
            head_copy(h).start()

        @pl.when(h == my_head)
        def _():
            got[c, me] = packed[h]

        return carry

    lax.fori_loop(0, HEADS, send_head, 0)

    def target_copy(n):
        side = lax.rem(n, 2)
        step = n // 2
        move = jnp.where(
            step == 0, 0, jnp.where(step == 1, -sig, jnp.where(step == 2, 2 * sig, -3 * sig))
        )
        return rcopy(
            tgt_ref,
            tgts.at[n],
            t_send.at[0],
            t_recv.at[0],
            xl=lax.rem(xl + side, 2),
            z=lax.rem(z + move + 8, 8),
        )

    def send_target(n, carry):
        target_copy(n).start()
        return carry

    lax.fori_loop(1, 8, send_target, 0)

    def arrival(g):
        def wait(count):
            part = got.at[c, pl.ds(4 * g, count)]
            rcopy(part, part, a_send.at[0], a_recv.at[g], xh=xh, y=y).wait_recv()

        @pl.when(g != my_group)
        def _():
            wait(4)

        @pl.when(g == my_group)
        def _():
            wait(3)

    def forward(g):
        part = got.at[c, pl.ds(4 * g, 4), pl.ds(0, ROWS)]
        return rcopy(part, part, f_send.at[g], f_recv.at[g], c=1 - c)

    def forwarded(g):
        part = got.at[1 - c, pl.ds(4 * g, 4), pl.ds(0, ROWS)]
        return rcopy(part, part, f_send.at[g], f_recv.at[g], c=1 - c)

    scale = LOG2E / math.sqrt(HEAD_DIM)

    def result_copy(i):
        return rcopy(
            outs.at[i],
            att.at[my_head],
            r_send.at[0],
            r_recv.at[0],
            xh=i // 8,
            y=lax.rem(i, 8),
        )

    def pair_of(gq, gk, masked):
        block = got[:, pl.ds(4 * gk, 4), 0:ROWS, :].reshape(CHUNK, ROWS)
        s = lax.dot_general(
            qt[gq], block, (((1,), (1,)), ((), ())), preferred_element_type=F32
        )
        if masked:
            shape = (SPAN, CHUNK)
            row = rows_of(shape)
            col = lanes(shape)
            later = col >= SPAN
            key = jnp.where(later, col - SPAN, col)
            key = key + (key // ROWS) * ROWS + jnp.where(later, ROWS, 0)
            s = jnp.where(key <= row + (row // ROWS) * ROWS + c * ROWS, s, NEGATIVE)
        s_scr[...] = s
        top = s[:, 0:ROWS]
        for g in range(1, CHUNK // ROWS):
            top = jnp.maximum(top, s[:, g * ROWS : (g + 1) * ROWS])
        old = mx_ref[gq]
        top = jnp.maximum(old, jnp.max(top, axis=1, keepdims=True) * scale)
        mx_ref[gq] = top
        factor = jnp.exp2(old - top)
        total = sum_ref[gq] * factor
        parts = []
        for g in range(CHUNK // ROWS):
            p = jnp.exp2(s_scr[:, g * ROWS : (g + 1) * ROWS] * scale - top)
            total = total + p
            parts.append(p.astype(BF16))
        sum_ref[gq] = total
        p = jnp.concatenate(parts, axis=1)
        pv_ref[gq] = pv_ref[gq] * factor + jnp.dot(p, block, preferred_element_type=F32)

    def finish(gq):
        out = pv_ref[gq] / jnp.sum(sum_ref[gq], axis=1, keepdims=True)
        for u in range(4):
            i = 4 * gq + u
            top_part = out[u * ROWS : u * ROWS + HEAD_DIM]
            bottom = out[u * ROWS + HEAD_DIM : (u + 1) * ROWS]
            whole = jnp.where(low_half, pltpu.roll(top_part, HEAD_DIM, 1), bottom).astype(BF16)
            outs[i] = whole

            @pl.when(i != me)
            def _():
                result_copy(i).start()

            @pl.when(i == me)
            def _():
                att[my_head] = whole

    def phase(p, carry):
        g = lax.rem(start + p, 4)
        arrival(g)
        forward(g).start()
        for u in range(4):
            qp = got[c, 4 * g + u, ROWS : ROWS + HEAD_DIM].astype(F32)
            qt[g, u * ROWS : u * ROWS + HEAD_DIM] = jnp.where(low_half, qp, 0.0).astype(BF16)
            qt[g, u * ROWS + HEAD_DIM : (u + 1) * ROWS] = jnp.where(
                low_half, pltpu.roll(qp, HEAD_DIM, 1), 0.0
            ).astype(BF16)
        mx_ref[g] = jnp.full((SPAN, ROWS), NEGATIVE, F32)
        sum_ref[g] = jnp.zeros((SPAN, ROWS), F32)
        pv_ref[g] = jnp.zeros((SPAN, ROWS), F32)
        forwarded(g).wait_recv()

        def visit(m, inner):
            other = lax.rem(start + m, 4)
            gq = jnp.maximum(g, other)
            gk = jnp.minimum(g, other)

            @pl.when(m < p)
            def _():
                pair_of(gq, gk, False)

            @pl.when(m == p)
            def _():
                pair_of(g, g, True)

            ready = jnp.where(gq < start, gq + 4 - start, jnp.where(start == 0, gq, 3))

            @pl.when(jnp.logical_and(p == ready, jnp.logical_or(m == p, gq != g)))
            def _():
                finish(gq)

            return inner

        lax.fori_loop(0, p + 1, visit, 0)
        return carry

    @pl.when(is_head)
    def _():
        lax.fori_loop(0, 4, phase, 0)

    swap.wait_recv()
    share = wide.at[half_rows, pl.ds(SHARE, SHARE)]
    pass_on = rcopy(share, share, w_sem.at[2], w_sem.at[3], c=1 - c)
    pass_on.start()

    @pl.when(is_head)
    def _():
        part = att.at[pl.ds(0, HEADS - 1)]
        rcopy(part, part, r_send.at[0], r_recv.at[0], xh=xh, y=y).wait_recv()

    @pl.when(jnp.logical_not(is_head))
    def _():
        rcopy(att, att, r_send.at[0], r_recv.at[0], xh=xh, y=y).wait_recv()

    for fetch in fetches[5:]:
        fetch.wait()
    for pair in range(HEADS // 2):
        at = slice(pair * ROWS, (pair + 1) * ROWS)
        even = att[2 * pair].astype(F32)
        odd = att[2 * pair + 1].astype(F32)
        attended[0:HEAD_DIM, at] = jnp.where(
            low_half, even, pltpu.roll(odd, HEAD_DIM, 1)
        ).astype(BF16)
        attended[HEAD_DIM:ROWS, at] = jnp.where(
            low_half, pltpu.roll(even, HEAD_DIM, 1), odd
        ).astype(BF16)
    residual = hid_ref[...].astype(F32) + jnp.dot(
        attended[...], ow_ref[...], preferred_element_type=F32
    )
    center = residual - jnp.sum(residual, axis=1, keepdims=True) * (1.0 / D)
    spread = jnp.sum(center * center, axis=1, keepdims=True) * (1.0 / D)
    rows_buf[0] = (center * lax.rsqrt(spread + NORM_EPSILON) * gain_ref[...].reshape(1, D)).astype(BF16)

    def row_copy(n):
        if n < 4:
            return rcopy(
                rows_buf.at[2 * n],
                rows_buf.at[2 * n + 1],
                c_send.at[n],
                c_recv.at[2 * n + 1],
                xl=1 - xl,
            )
        if n == 4:
            return rcopy(rows_buf.at[0], rows_buf.at[2], c_send.at[4], c_recv.at[2], z=z_dn)
        if n == 5:
            return rcopy(rows_buf.at[0], relay.at[0], c_send.at[5], c_recv.at[8], z=z_up)
        if n == 6:
            return rcopy(rows_buf.at[2], relay.at[1], c_send.at[6], c_recv.at[9], z=z_up)
        if n == 7:
            return rcopy(relay.at[0], rows_buf.at[4], c_send.at[7], c_recv.at[4], z=z_dn)
        return rcopy(relay.at[1], rows_buf.at[6], c_send.at[8], c_recv.at[6], z=z_dn)

    def row_wait(slot):
        ref = relay.at[slot - 8] if slot >= 8 else rows_buf.at[slot]
        rcopy(rows_buf.at[0], ref, c_send.at[0], c_recv.at[slot], z=z_dn).wait_recv()

    row_copy(4).start()
    row_copy(5).start()
    row_copy(0).start()
    mine.wait()
    pass_on.wait_recv()

    part = tgts.at[pl.ds(1, 7)]
    rcopy(part, part, t_send.at[0], t_recv.at[0], z=z_dn).wait_recv()
    diagonal = lane == rows_of((ROWS, ROWS))
    other = xl * 8 + z_pair

    def stat_copy(slot):
        side = lax.rem(slot, 2)
        back = lax.rem(z - sig * (slot // 2) + 8, 8)
        return rcopy(
            stat_out.at[slot],
            stats.at[xl * 4 + z // 2],
            s_send.at[0],
            s_recv.at[0],
            xl=lax.rem(xl + side, 2),
            z=back,
        )

    def as_row(column):
        return jnp.sum(jnp.where(diagonal, column, 0.0), axis=0, keepdims=True)

    def score_rows(n, carry):
        @pl.when(n == 0)
        def _():
            row_wait(1)
            row_wait(2)
            row_copy(6).start()
            row_copy(1).start()
            row_wait(8)
            row_copy(7).start()

        @pl.when(n == 1)
        def _():
            row_wait(9)
            row_copy(8).start()
            row_wait(4)
            row_copy(2).start()
            row_wait(3)

        @pl.when(n == 2)
        def _():
            row_wait(6)
            row_copy(3).start()
            row_wait(5)

        @pl.when(n == 3)
        def _():
            row_wait(7)

        block = rows_buf[pl.ds(2 * n, 2)].reshape(2 * ROWS, D)
        top = jnp.full((2 * ROWS, ROWS), NEGATIVE, F32)
        for k in range(TILES):
            s = jnp.dot(
                block, wide[:, k * TILE : (k + 1) * TILE], preferred_element_type=F32
            )
            logit[k] = s
            top = jnp.maximum(top, jnp.maximum(s[:, :ROWS], s[:, ROWS:]))

        def placed(slot):
            wanted = jnp.broadcast_to(tgts[slot], (ROWS, ROWS))
            wanted = jnp.sum(
                jnp.where(diagonal, wanted.astype(F32), 0.0), axis=1, keepdims=True
            ).astype(jnp.int32)
            here = wanted - doc * SHARE
            there = wanted - other * SHARE
            spot = jnp.where(
                jnp.logical_and(here >= 0, here < SHARE),
                here,
                jnp.where(jnp.logical_and(there >= 0, there < SHARE), there + SHARE, -1),
            )
            return jnp.broadcast_to(spot, (ROWS, ROWS)) - lane

        place = jnp.concatenate([placed(2 * n), placed(2 * n + 1)], axis=0)
        top = jnp.max(top, axis=1, keepdims=True)
        top2 = jnp.broadcast_to(top * LOG2E, (2 * ROWS, ROWS))
        sum_ref[0, 0 : 2 * ROWS] = jnp.zeros((2 * ROWS, ROWS), F32)
        pv_ref[0, 0 : 2 * ROWS] = jnp.zeros((2 * ROWS, ROWS), F32)

        def add_up(k, inner):
            total = sum_ref[0, 0 : 2 * ROWS]
            pick = pv_ref[0, 0 : 2 * ROWS]
            for g in range(TILE // ROWS):
                s = logit[k, :, g * ROWS : (g + 1) * ROWS]
                total = total + jnp.exp2(s * LOG2E - top2)
                pick = pick + jnp.where(place == k * TILE + g * ROWS, s, 0.0)
            sum_ref[0, 0 : 2 * ROWS] = total
            pv_ref[0, 0 : 2 * ROWS] = pick
            return inner

        lax.fori_loop(0, TILES, add_up, 0)
        lse = top + jnp.log(jnp.sum(sum_ref[0, 0 : 2 * ROWS], axis=1, keepdims=True))
        pick = jnp.sum(pv_ref[0, 0 : 2 * ROWS], axis=1, keepdims=True)
        row8 = rows_of((8, ROWS))
        tiles = [
            jnp.where(row8 == 0, as_row(lse[at : at + ROWS]), as_row(pick[at : at + ROWS]))
            for at in (0, ROWS)
        ]
        stat_out[2 * n + 1] = tiles[1]
        stat_copy(2 * n + 1).start()

        @pl.when(n != 0)
        def _():
            stat_out[2 * n] = tiles[0]
            stat_copy(2 * n).start()

        @pl.when(n == 0)
        def _():
            stats[xl * 4 + z // 2] = tiles[0]

        return carry

    lax.fori_loop(0, 4, score_rows, 0)

    part = stats.at[pl.ds(0, 7)]
    rcopy(part, part, s_send.at[0], s_recv.at[0], z=z_dn).wait_recv()
    parts = [stats[n] for n in range(8)]
    top = parts[0][0:1]
    for part in parts[1:]:
        top = jnp.maximum(top, part[0:1])
    total = jnp.zeros((1, ROWS), F32)
    pick = jnp.zeros((1, ROWS), F32)
    for part in parts:
        total = total + jnp.exp(part[0:1] - top)
        pick = pick + part[1:2]
    place = seq * ROWS + lanes((1, ROWS))
    nll = jnp.where(place < lengths_ref[doc], top + jnp.log(total) - pick, 0.0)
    seqs[seq] = jnp.broadcast_to(jnp.sum(nll, axis=1, keepdims=True), (1, ROWS))

    for k in range(1, SEQ):
        rcopy(seqs.at[seq], seqs.at[seq], q_send.at[0], q_recv.at[0], **peer_seq(k)).start()

    @pl.when(is_head)
    def _():
        part = packed.at[pl.ds(0, HEADS - 1)]
        rcopy(part, part, a_send.at[0], a_recv.at[0], xh=xh, y=y).wait_send()
        part = outs.at[pl.ds(0, 15)]
        rcopy(part, part, r_send.at[0], r_recv.at[0], xh=xh, y=y).wait_send()
        for g in range(4):
            forward(g).wait_send()

    @pl.when(jnp.logical_not(is_head))
    def _():
        rcopy(packed, packed, a_send.at[0], a_recv.at[0], xh=xh, y=y).wait_send()

    swap.wait_send()
    pass_on.wait_send()
    for n in range(9):
        row_copy(n).wait_send()
    part = tgts.at[pl.ds(1, 7)]
    rcopy(part, part, t_send.at[0], t_recv.at[0], z=z_dn).wait_send()
    part = stat_out.at[pl.ds(1, 7)]
    rcopy(part, part, s_send.at[0], s_recv.at[0], z=z_dn).wait_send()
    others = seqs.at[pl.ds(0, SEQ - 1)]
    rcopy(others, others, q_send.at[0], q_recv.at[0], z=z_dn).wait_recv()
    docs[doc] = jnp.sum(seqs[...], axis=0)

    for k in range(1, DOCS):
        rcopy(docs.at[doc], docs.at[doc], d_send.at[0], d_recv.at[0], **peer_doc(k)).start()
    rcopy(others, others, q_send.at[0], q_recv.at[0], z=z_dn).wait_send()
    part = docs.at[pl.ds(0, DOCS - 1)]
    rcopy(part, part, d_send.at[0], d_recv.at[0], z=z_dn).wait_recv()

    shape = (DOCS, ROWS)
    row = rows_of(shape)
    col = lanes(shape)
    column = docs[...].reshape(DOCS, ROWS)
    for d in range(DOCS):
        column = jnp.where(row == d, column / lengths_ref[d].astype(F32), column)
    valid = lanes((1, ROWS)) < DOCS
    line = jnp.sum(jnp.where(row == col, column, 0.0), axis=0, keepdims=True)
    mean = jnp.sum(line, axis=1, keepdims=True) * (1.0 / DOCS)
    off = jnp.where(valid, line - mean, 0.0)
    spread = jnp.sqrt(jnp.sum(off * off, axis=1, keepdims=True) * (1.0 / DOCS) + SPREAD_EPSILON)
    ahead = jnp.logical_or(
        column < line, jnp.logical_and(column == line, row < col)
    )
    rank = jnp.sum(jnp.where(ahead, 1.0, 0.0), axis=0, keepdims=True)
    scaled = rank_ref[0] * (DOCS - 1)
    low_index = lax.div(scaled, 99)
    high_index = jnp.minimum(low_index + 1, DOCS - 1)
    fraction = (scaled - 99 * low_index).astype(F32) / 99.0
    hit_low = jnp.logical_and(valid, rank == low_index.astype(F32))
    hit_high = jnp.logical_and(valid, rank == high_index.astype(F32))
    low_value = jnp.sum(jnp.where(hit_low, line, 0.0), axis=1, keepdims=True)
    high_value = jnp.sum(jnp.where(hit_high, line, 0.0), axis=1, keepdims=True)
    level = (1.0 - fraction) * low_value + fraction * high_value
    accepted = jax.nn.sigmoid((level - line) / spread)
    row = rows_of((8, ROWS))
    final_ref[...] = jnp.where(row == 0, nll, jnp.where(row == 1, line, accepted))
    rcopy(part, part, d_send.at[0], d_recv.at[0], z=z_dn).wait_send()


def split_kernel(final_ref, nll_ref, ppl_ref, acc_ref):
    nll_ref[...] = final_ref[0:1]
    ppl_ref[...] = final_ref[1:2, :DOCS]
    acc_ref[...] = final_ref[2:3, :DOCS]


def turn_tables():
    spot = np.arange(ROWS) % HEAD_DIM
    freq = ROTARY_BASE ** (-2.0 * (spot % (ROT // 2)) / ROT)
    freq = np.where(spot < ROT, freq, 0.0)
    base = np.arange(SEQ)[:, None] * float(ROWS) * freq[None, :]
    step = np.arange(ROWS)[:, None] * freq[None, :]
    base = np.stack([np.cos(base), np.sin(base)], axis=1).astype(np.float32)
    step = np.stack([np.cos(step), np.sin(step)], axis=0).astype(np.float32)
    return base, step


def shards(
    hidden,
    queries,
    key_states,
    values,
    targets,
    lengths,
    keep_rank,
    out_weight,
    final_gain,
    unembed,
):
    base, step = turn_tables()
    vmem = pl.BlockSpec(memory_space=pltpu.VMEM)
    dma = pltpu.SemaphoreType.DMA
    final = pl.pallas_call(
        kernel,
        name="scoring",
        out_shape=jax.ShapeDtypeStruct((8, ROWS), F32),
        in_specs=[pl.BlockSpec(memory_space=pltpu.HBM)] * 12,
        out_specs=vmem,
        scratch_shapes=[
            pltpu.VMEM((2, ROWS), F32),
            pltpu.VMEM((2, ROWS, ROWS), F32),
            pltpu.SMEM((DOCS,), jnp.int32),
            pltpu.SMEM((1,), jnp.int32),
            pltpu.VMEM((ROWS, D), BF16),
            pltpu.VMEM((ROWS, D), BF16),
            pltpu.VMEM((ROWS, D), BF16),
            pltpu.VMEM((ROWS, D), BF16),
            pltpu.VMEM((D,), F32),
            pltpu.VMEM((D, D), BF16),
            pltpu.VMEM((HEADS, ROWS + HEAD_DIM, ROWS), BF16),
            pltpu.VMEM((2, 16, ROWS + HEAD_DIM, ROWS), BF16),
            pltpu.VMEM((16, HEAD_DIM, ROWS), BF16),
            pltpu.VMEM((HEADS, HEAD_DIM, ROWS), BF16),
            pltpu.VMEM((ROWS, D), BF16),
            pltpu.VMEM((4, SPAN, ROWS), BF16),
            pltpu.VMEM((SPAN, CHUNK), F32),
            pltpu.VMEM((4, SPAN, ROWS), F32),
            pltpu.VMEM((4, SPAN, ROWS), F32),
            pltpu.VMEM((4, SPAN, ROWS), F32),
            pltpu.VMEM((D, WIDE), BF16),
            pltpu.VMEM((8, ROWS, D), BF16),
            pltpu.VMEM((2, ROWS, D), BF16),
            pltpu.VMEM((TILES, 2 * ROWS, TILE), F32),
            pltpu.VMEM((8, 1, ROWS), jnp.int32),
            pltpu.VMEM((8, 8, ROWS), F32),
            pltpu.VMEM((8, 8, ROWS), F32),
            pltpu.VMEM((SEQ, 1, ROWS), F32),
            pltpu.VMEM((DOCS, 1, ROWS), F32),
            dma((1,)),
            dma((4,)),
            dma((4,)),
            dma((4,)),
            dma((1,)),
            dma((1,)),
            dma((5,)),
            dma((9,)),
            dma((10,)),
            dma((1,)),
            dma((1,)),
            dma((1,)),
            dma((1,)),
            dma((1,)),
            dma((1,)),
            dma((1,)),
            dma((1,)),
            dma((11,)),
        ],
        compiler_params=pltpu.CompilerParams(
            collective_id=0, has_side_effects=True, vmem_limit_bytes=67043328
        ),
    )(
        jnp.asarray(base),
        jnp.asarray(step),
        lengths,
        keep_rank,
        queries[0],
        key_states[0],
        values[0],
        hidden[0],
        targets,
        final_gain,
        out_weight,
        unembed,
    )
    nll, ppl, acceptance = pl.pallas_call(
        split_kernel,
        name="split",
        out_shape=(
            jax.ShapeDtypeStruct((1, ROWS), F32),
            jax.ShapeDtypeStruct((1, DOCS), F32),
            jax.ShapeDtypeStruct((1, DOCS), F32),
        ),
        in_specs=[vmem],
        out_specs=(vmem, vmem, vmem),
    )(final)
    return (nll, ppl.reshape(DOCS), acceptance.reshape(DOCS))


def solution(mesh):
    split = Mesh(mesh.devices.reshape(2, 8, 2, 2, 8), ("xh", "y", "c", "xl", "z"))
    rows = ("xh", "y", "c")
    parts = ("xl", "z")
    placed = (
        P(parts, rows, None),
        P(parts, rows, None),
        P(parts, rows, None),
        P(parts, rows, None),
        P(parts, rows),
        P(),
        P(),
        P(),
        P(),
        P(None, parts),
    )
    return jax.shard_map(
        shards, mesh=split, in_specs=placed, out_specs=(P(parts, rows), P(), P()), check_vma=False
    )
```

```python
import math

import jax
import jax.numpy as jnp
import numpy as np
from jax import lax
from jax.experimental import pallas as pl
from jax.experimental.pallas import tpu as pltpu
from jax.sharding import Mesh
from jax.sharding import PartitionSpec as P

HEADS = 12
HEAD_DIM = 64
ROT = 16
D = 768
ROWS = 128
SHARE = 1664
WIDE = 2 * SHARE
TILE = 256
TILES = WIDE // TILE
DOCS = 16
SEQ = 32
HALF = 256
SPAN = 512
NEGATIVE = -1e30
ROTARY_BASE = 10000.0
NORM_EPSILON = 1e-05
SPREAD_EPSILON = 0.0001
LOG2E = 1.4426950408889634
MESH = pl.DeviceIdType.MESH
F32 = jnp.float32
BF16 = jnp.bfloat16


def lanes(shape):
    return lax.broadcasted_iota(jnp.int32, shape, len(shape) - 1)


def rows_of(shape):
    return lax.broadcasted_iota(jnp.int32, shape, len(shape) - 2)


def rcopy(src, dst, ss, rs, **where):
    return pltpu.make_async_remote_copy(
        src_ref=src,
        dst_ref=dst,
        send_sem=ss,
        recv_sem=rs,
        device_id=where,
        device_id_type=MESH,
    )


def kernel(
    base_in,
    step_in,
    lengths_in,
    rank_in,
    q_in,
    k_in,
    v_in,
    hid_in,
    tgt_ref,
    gain_in,
    ow_in,
    un_ref,
    final_ref,
    base_ref,
    step_ref,
    lengths_ref,
    rank_ref,
    q_ref,
    k_ref,
    v_ref,
    hid_ref,
    gain_ref,
    ow_ref,
    packed,
    got,
    outs,
    att,
    qt,
    vt,
    s_scr,
    mx_ref,
    sum_ref,
    pv_ref,
    v_sum,
    v_pick,
    wide,
    rows_buf,
    relay,
    logit,
    tgts,
    stat_out,
    stats,
    seqs,
    a_send,
    a_recv,
    f_send,
    f_recv,
    r_send,
    r_recv,
    w_sem,
    c_send,
    c_recv,
    t_send,
    t_recv,
    s_send,
    s_recv,
    q_send,
    q_recv,
    i_sem,
    tie_buf,
    tie_sem,
):
    xh = lax.axis_index("xh")
    y = lax.axis_index("y")
    c = lax.axis_index("c")
    xl = lax.axis_index("xl")
    z = lax.axis_index("z")
    me = xh * 8 + y
    seq = me * 2 + c
    doc = xl * 8 + z
    sig = 1 - 2 * lax.rem(z, 2)
    z_up = lax.rem(z + sig + 8, 8)
    z_dn = lax.rem(z - sig + 8, 8)
    z_pair = z + sig

    barrier = pltpu.get_barrier_semaphore()

    def peer_seq(k):
        n = lax.rem(seq + k, SEQ)
        return {"xh": lax.div(n, 16), "y": lax.rem(lax.div(n, 2), 8), "c": lax.rem(n, 2)}

    def peer_doc(k):
        n = lax.rem(doc + k, DOCS)
        return {"xl": lax.div(n, 8), "z": lax.rem(n, 8)}

    for k in range(1, SEQ):
        pl.semaphore_signal(barrier, inc=1, device_id=peer_seq(k), device_id_type=MESH)
    for k in range(1, DOCS):
        pl.semaphore_signal(barrier, inc=1, device_id=peer_doc(k), device_id_type=MESH)

    fetches = [
        pltpu.make_async_copy(src, dst, i_sem.at[n])
        for n, (src, dst) in enumerate(
            (
                (base_in.at[seq], base_ref),
                (step_in, step_ref),
                (k_in, k_ref),
                (q_in, q_ref),
                (v_in, v_ref),
                (hid_in, hid_ref),
                (ow_in, ow_ref),
                (gain_in, gain_ref),
                (lengths_in, lengths_ref),
                (rank_in, rank_ref),
                (tgt_ref, tgts.at[0]),
            )
        )
    ]
    for fetch in fetches:
        fetch.start()
    mine = pltpu.make_async_copy(un_ref, wide.at[:, pl.ds(0, SHARE)], w_sem.at[4])
    mine.start()

    lane = lanes((ROWS, ROWS))
    low = lane < HEAD_DIM
    first = lax.rem(lane, HEAD_DIM) < ROT // 2
    low_half = low[:HEAD_DIM]

    for fetch in fetches[:5]:
        fetch.wait()

    base_cos = base_ref[0:1]
    base_sin = base_ref[1:2]
    cosine = base_cos * step_ref[0] - base_sin * step_ref[1]
    sine = base_sin * step_ref[0] + base_cos * step_ref[1]
    sine = jnp.where(first, -sine, sine)

    def turn(block):
        partner = jnp.where(first, pltpu.roll(block, ROWS - 8, 1), pltpu.roll(block, 8, 1))
        return block * cosine + partner * sine

    for pair in range(HEADS // 2):
        at = slice(pair * ROWS, (pair + 1) * ROWS)
        tk = turn(k_ref[:, at].astype(F32))
        tq = turn(q_ref[:, at].astype(F32))
        tv = v_ref[:, at].astype(F32)
        rk = pltpu.roll(tk, HEAD_DIM, 1)
        rq = pltpu.roll(tq, HEAD_DIM, 1)
        rv = pltpu.roll(tv, HEAD_DIM, 1)
        packed[2 * pair, 0:ROWS] = jnp.where(low, tk, rv).astype(BF16)
        packed[2 * pair + 1, 0:ROWS] = jnp.where(low, rk, tv).astype(BF16)
        packed[2 * pair, ROWS : ROWS + HEAD_DIM] = jnp.where(
            low_half, tq[:HEAD_DIM], rq[HEAD_DIM:]
        ).astype(BF16)
        packed[2 * pair + 1, ROWS : ROWS + HEAD_DIM] = jnp.where(
            low_half, rq[:HEAD_DIM], tq[HEAD_DIM:]
        ).astype(BF16)

    pl.semaphore_wait(barrier, SEQ - 1 + DOCS - 1)

    half_rows = pl.ds(pl.multiple_of(c * (D // 2), D // 2), D // 2)
    swap = rcopy(
        un_ref.at[half_rows],
        wide.at[half_rows, pl.ds(SHARE, SHARE)],
        w_sem.at[0],
        w_sem.at[1],
        z=z_pair,
    )
    swap.start()

    is_head = jnp.logical_and(y != 3, y != 7)
    my_slot = y - jnp.where(y > 3, 1, 0)
    my_head = jnp.where(is_head, xh * 6 + my_slot, -1)

    start = lax.rem(my_head, 4)
    my_group = lax.div(me, 4)

    def head_copy(h):
        yi = lax.rem(h, 6)
        return rcopy(
            packed.at[h],
            got.at[c, me],
            a_send.at[0],
            a_recv.at[my_group],
            xh=h // 6,
            y=yi + jnp.where(yi > 2, 1, 0),
        )

    tie_y = lax.rem(y + 4, 8)
    has_tie = jnp.logical_and(tie_y != 3, tie_y != 7)
    tie_head = jnp.where(has_tie, xh * 6 + tie_y - jnp.where(tie_y > 3, 1, 0), -1)
    tie_from = xh * 8 + lax.rem(y + 3, 8)
    relays = jnp.logical_and(y != 4, y != 0)
    tie_send = rcopy(
        packed.at[jnp.maximum(tie_head, 0)],
        tie_buf,
        a_send.at[0],
        tie_sem.at[0],
        xh=xh,
        y=lax.rem(y + 5, 8),
    )
    tie_pass = rcopy(
        tie_buf,
        got.at[c, tie_from],
        tie_sem.at[1],
        a_recv.at[lax.div(tie_from, 4)],
        xh=xh,
        y=lax.rem(y + 7, 8),
    )

    @pl.when(has_tie)
    def _():
        tie_send.start()

    def send_head(n, carry):
        h = 4 * lax.rem(n + me, 3) + lax.rem(my_group + 4 - n // 3, 4)

        @pl.when(jnp.logical_and(h != my_head, h != tie_head))
        def _():
            head_copy(h).start()

        @pl.when(h == my_head)
        def _():
            got[c, me] = packed[h]

        return carry

    lax.fori_loop(0, HEADS, send_head, 0)

    def target_copy(n):
        side = lax.rem(n, 2)
        step = n // 2
        move = jnp.where(
            step == 0, 0, jnp.where(step == 1, -sig, jnp.where(step == 2, 2 * sig, -3 * sig))
        )
        return rcopy(
            tgt_ref,
            tgts.at[n],
            t_send.at[0],
            t_recv.at[0],
            xl=lax.rem(xl + side, 2),
            z=lax.rem(z + move + 8, 8),
        )

    def send_target(n, carry):
        target_copy(n).start()
        return carry

    lax.fori_loop(1, 8, send_target, 0)

    @pl.when(relays)
    def _():
        tie_send.wait_recv()
        tie_pass.start()

    def arrival(g):
        def wait(count):
            part = got.at[c, pl.ds(4 * g, count)]
            rcopy(part, part, a_send.at[0], a_recv.at[g], xh=xh, y=y).wait_recv()

        @pl.when(g != my_group)
        def _():
            wait(4)

        @pl.when(g == my_group)
        def _():
            wait(3)

    def forward(g):
        part = got.at[c, pl.ds(4 * g, 4), pl.ds(0, ROWS)]
        return rcopy(part, part, f_send.at[g], f_recv.at[g], c=1 - c)

    def forwarded(g):
        part = got.at[1 - c, pl.ds(4 * g, 4), pl.ds(0, ROWS)]
        return rcopy(part, part, f_send.at[g], f_recv.at[g], c=1 - c)

    scale = LOG2E / math.sqrt(HEAD_DIM)

    def result_copy(i):
        return rcopy(
            outs.at[i],
            att.at[my_head],
            r_send.at[0],
            r_recv.at[0],
            xh=i // 8,
            y=lax.rem(i, 8),
        )

    def pair_of(gq, gk, diagonal):
        blocks = [(uh, par) for uh in range(2) for par in range(2)]
        tops = []
        for hq in range(2):
            queries = qt[gq, hq * HALF : (hq + 1) * HALF]
            top = jnp.full((8, HALF), NEGATIVE, F32)
            for b, (uh, par) in enumerate(blocks):
                if diagonal and uh > hq:
                    continue
                keys = got[par, pl.ds(4 * gk + 2 * uh, 2), 0:ROWS, :].reshape(HALF, ROWS)
                s = lax.dot_general(
                    keys, queries, (((1,), (1,)), ((), ())), preferred_element_type=F32
                )
                if diagonal and uh == hq:
                    row = rows_of((HALF, HALF))
                    col = lanes((HALF, HALF))
                    key = row + jnp.where(row >= ROWS, ROWS, 0) + par * ROWS
                    query = col + jnp.where(col >= ROWS, ROWS, 0) + c * ROWS
                    s = jnp.where(key <= query, s, NEGATIVE)
                s_scr[hq, b] = s
                top = jnp.maximum(top, jnp.max(s.reshape(HALF // 8, 8, HALF), axis=0))
            tops.append(top)
        for hq in range(2):
            old = mx_ref[gq, hq]
            new = jnp.maximum(old, jnp.max(tops[hq], axis=0, keepdims=True) * scale)
            mx_ref[gq, hq] = new
            factor = jnp.exp2(old - new)
            total = sum_ref[gq, hq] * factor
            parts = []
            count = 2 if diagonal and hq == 0 else 4
            for b in range(count):
                p = jnp.exp2(s_scr[hq, b] * scale - new)
                total = total + jnp.sum(p.reshape(HALF // 8, 8, HALF), axis=0)
                parts.append(p.astype(BF16))
            sum_ref[gq, hq] = total
            pv_ref[gq, hq] = pv_ref[gq, hq] * factor + jnp.dot(
                vt[gk, :, 0 : count * HALF],
                jnp.concatenate(parts, axis=0),
                preferred_element_type=F32,
            )

    def finish(gq):
        for hq in range(2):
            out = pv_ref[gq, hq] / jnp.sum(sum_ref[gq, hq], axis=0, keepdims=True)
            for u in range(2):
                i = 4 * gq + 2 * hq + u
                whole = out[:, u * ROWS : (u + 1) * ROWS].astype(BF16)
                outs[i] = whole

                @pl.when(i != me)
                def _():
                    result_copy(i).start()

                @pl.when(i == me)
                def _():
                    att[my_head] = whole

    def phase(p, carry):
        g = lax.rem(start + p, 4)
        for u in range(4):
            qp = got[c, 4 * g + u, ROWS : ROWS + HEAD_DIM].astype(F32)
            qt[g, u * ROWS : u * ROWS + HEAD_DIM] = jnp.where(low_half, qp, 0.0).astype(BF16)
            qt[g, u * ROWS + HEAD_DIM : (u + 1) * ROWS] = jnp.where(
                low_half, pltpu.roll(qp, HEAD_DIM, 1), 0.0
            ).astype(BF16)
        mx_ref[g] = jnp.full((2, 1, HALF), NEGATIVE, F32)
        sum_ref[g] = jnp.zeros((2, 8, HALF), F32)
        pv_ref[g] = jnp.zeros((2, HEAD_DIM, HALF), F32)
        forwarded(g).wait_recv()
        for uh in range(2):
            for par in range(2):
                block = got[par, pl.ds(4 * g + 2 * uh, 2), 0:ROWS, :].reshape(HALF, ROWS)
                turned = jnp.transpose(block.astype(F32))[HEAD_DIM:]
                at = (2 * uh + par) * HALF
                vt[g, :, at : at + HALF] = turned.astype(BF16)

        def visit(m, inner):
            other = lax.rem(start + m, 4)
            gq = jnp.maximum(g, other)
            gk = jnp.minimum(g, other)

            @pl.when(m < p)
            def _():
                pair_of(gq, gk, False)

            @pl.when(m == p)
            def _():
                pair_of(g, g, True)

            ready = jnp.where(gq < start, gq + 4 - start, jnp.where(start == 0, gq, 3))

            @pl.when(jnp.logical_and(p == ready, jnp.logical_or(m == p, gq != g)))
            def _():
                finish(gq)

            @pl.when(jnp.logical_and(m == 0, p < 3))
            def _():
                ahead = lax.rem(start + p + 1, 4)
                arrival(ahead)
                forward(ahead).start()

            return inner

        lax.fori_loop(0, p + 1, visit, 0)
        return carry

    @pl.when(is_head)
    def _():
        arrival(start)
        forward(start).start()
        lax.fori_loop(0, 4, phase, 0)

    @pl.when(is_head)
    def _():
        part = att.at[pl.ds(0, HEADS - 1)]
        rcopy(part, part, r_send.at[0], r_recv.at[0], xh=xh, y=y).wait_recv()

    @pl.when(jnp.logical_not(is_head))
    def _():
        rcopy(att, att, r_send.at[0], r_recv.at[0], xh=xh, y=y).wait_recv()

    for fetch in fetches[5:]:
        fetch.wait()
    residual = hid_ref[...].astype(F32) + lax.dot_general(
        att[...].reshape(D, ROWS),
        ow_ref[...],
        (((0,), (0,)), ((), ())),
        preferred_element_type=F32,
    )
    center = residual - jnp.sum(residual, axis=1, keepdims=True) * (1.0 / D)
    spread = jnp.sum(center * center, axis=1, keepdims=True) * (1.0 / D)
    rows_buf[0] = (center * lax.rsqrt(spread + NORM_EPSILON) * gain_ref[...].reshape(1, D)).astype(BF16)

    def row_copy(n):
        if n < 4:
            return rcopy(
                rows_buf.at[2 * n],
                rows_buf.at[2 * n + 1],
                c_send.at[n],
                c_recv.at[2 * n + 1],
                xl=1 - xl,
            )
        if n == 4:
            return rcopy(rows_buf.at[0], rows_buf.at[2], c_send.at[4], c_recv.at[2], z=z_dn)
        if n == 5:
            return rcopy(rows_buf.at[0], relay.at[0], c_send.at[5], c_recv.at[8], z=z_up)
        if n == 6:
            return rcopy(rows_buf.at[2], relay.at[1], c_send.at[6], c_recv.at[9], z=z_up)
        if n == 7:
            return rcopy(relay.at[0], rows_buf.at[4], c_send.at[7], c_recv.at[4], z=z_dn)
        return rcopy(relay.at[1], rows_buf.at[6], c_send.at[8], c_recv.at[6], z=z_dn)

    def row_wait(slot):
        ref = relay.at[slot - 8] if slot >= 8 else rows_buf.at[slot]
        rcopy(rows_buf.at[0], ref, c_send.at[0], c_recv.at[slot], z=z_dn).wait_recv()

    row_copy(4).start()
    row_copy(5).start()
    row_copy(0).start()
    swap.wait_recv()
    share = wide.at[half_rows, pl.ds(SHARE, SHARE)]
    pass_on = rcopy(share, share, w_sem.at[2], w_sem.at[3], c=1 - c)
    pass_on.start()
    mine.wait()
    pass_on.wait_recv()

    part = tgts.at[pl.ds(1, 7)]
    rcopy(part, part, t_send.at[0], t_recv.at[0], z=z_dn).wait_recv()
    diagonal = lane == rows_of((ROWS, ROWS))
    other = xl * 8 + z_pair

    slot_j = (xl * 4 + z // 2) * 8

    def as_row(column):
        return jnp.sum(jnp.where(diagonal, column, 0.0), axis=0, keepdims=True)

    def score_rows(n, carry):
        @pl.when(n == 0)
        def _():
            row_wait(1)
            row_wait(2)
            row_copy(6).start()
            row_copy(1).start()
            row_wait(8)
            row_copy(7).start()

        @pl.when(n == 1)
        def _():
            row_wait(9)
            row_copy(8).start()
            row_wait(4)
            row_copy(2).start()
            row_wait(3)

        @pl.when(n == 2)
        def _():
            row_wait(6)
            row_copy(3).start()
            row_wait(5)

        @pl.when(n == 3)
        def _():
            row_wait(7)

        block = rows_buf[pl.ds(2 * n, 2)].reshape(2 * ROWS, D)
        top = jnp.full((2 * ROWS, ROWS), NEGATIVE, F32)
        for k in range(TILES):
            s = jnp.dot(
                block, wide[:, k * TILE : (k + 1) * TILE], preferred_element_type=F32
            )
            logit[k] = s
            top = jnp.maximum(top, jnp.maximum(s[:, :ROWS], s[:, ROWS:]))

        def placed(slot):
            wanted = jnp.broadcast_to(tgts[slot], (ROWS, ROWS))
            wanted = jnp.sum(
                jnp.where(diagonal, wanted.astype(F32), 0.0), axis=1, keepdims=True
            ).astype(jnp.int32)
            here = wanted - doc * SHARE
            there = wanted - other * SHARE
            spot = jnp.where(
                jnp.logical_and(here >= 0, here < SHARE),
                here,
                jnp.where(jnp.logical_and(there >= 0, there < SHARE), there + SHARE, -1),
            )
            return jnp.broadcast_to(spot, (ROWS, ROWS)) - lane

        place = jnp.concatenate([placed(2 * n), placed(2 * n + 1)], axis=0)
        top = jnp.max(top, axis=1, keepdims=True)
        top2 = jnp.broadcast_to(top * LOG2E, (2 * ROWS, ROWS))
        v_sum[...] = jnp.zeros((2 * ROWS, ROWS), F32)
        v_pick[...] = jnp.zeros((2 * ROWS, ROWS), F32)

        def add_up(k, inner):
            total = v_sum[...]
            pick = v_pick[...]
            for g in range(TILE // ROWS):
                s = logit[k, :, g * ROWS : (g + 1) * ROWS]
                total = total + jnp.exp2(s * LOG2E - top2)
                pick = pick + jnp.where(place == k * TILE + g * ROWS, s, 0.0)
            v_sum[...] = total
            v_pick[...] = pick
            return inner

        lax.fori_loop(0, TILES, add_up, 0)
        lse = top + jnp.log(jnp.sum(v_sum[...], axis=1, keepdims=True))
        pick = jnp.sum(v_pick[...], axis=1, keepdims=True)
        row2 = rows_of((2, ROWS))
        for side in range(2):
            at = slice(side * ROWS, (side + 1) * ROWS)
            stat_out[n, lax.rem(xl + side, 2)] = jnp.where(
                row2 == 0, as_row(lse[at]), as_row(pick[at])
            )
        spot = slot_j + lax.rem(z - sig * n + 8, 8)
        stats[spot] = stat_out[n]
        for k in range(1, DOCS):
            rcopy(
                stat_out.at[n], stats.at[spot], s_send.at[0], s_recv.at[0], **peer_doc(k)
            ).start()

        return carry

    lax.fori_loop(0, 4, score_rows, 0)

    sent = stats.at[pl.ds(0, 60)]
    rcopy(sent, sent, s_send.at[0], s_recv.at[0], z=z_dn).wait_recv()
    entries = stats[...].reshape(8, DOCS, 2, ROWS)
    top = jnp.max(entries, axis=0)
    total = jnp.sum(jnp.exp(entries - top[None]), axis=0)
    pick = jnp.sum(entries, axis=0)
    shape = (DOCS, ROWS)
    row = rows_of(shape)
    col = lanes(shape)
    scored = jnp.where(
        rows_of((DOCS, 2, ROWS)) == 0, top + jnp.log(total), -pick
    )
    scored = jnp.sum(scored, axis=1)
    limit = jnp.zeros(shape, jnp.int32)
    for d in range(DOCS):
        limit = jnp.where(row == d, lengths_ref[(d % 2) * 8 + d // 2], limit)
    scored = jnp.where(seq * ROWS + col < limit, scored, 0.0)
    nll = jnp.sum(jnp.where(row == 2 * z + xl, scored, 0.0), axis=0, keepdims=True)
    doc_of = lax.rem(row, 2) * 8 + lax.div(row, 2)
    sums = jnp.sum(scored, axis=1, keepdims=True)
    seqs[seq] = jnp.sum(jnp.where(col == doc_of, sums, 0.0), axis=0, keepdims=True)

    for k in range(1, SEQ):
        rcopy(seqs.at[seq], seqs.at[seq], q_send.at[0], q_recv.at[0], **peer_seq(k)).start()

    @pl.when(is_head)
    def _():
        part = packed.at[pl.ds(0, HEADS - 1)]
        rcopy(part, part, a_send.at[0], a_recv.at[0], xh=xh, y=y).wait_send()
        part = outs.at[pl.ds(0, 15)]
        rcopy(part, part, r_send.at[0], r_recv.at[0], xh=xh, y=y).wait_send()
        for g in range(4):
            forward(g).wait_send()

    @pl.when(jnp.logical_not(is_head))
    def _():
        rcopy(packed, packed, a_send.at[0], a_recv.at[0], xh=xh, y=y).wait_send()

    @pl.when(relays)
    def _():
        tie_pass.wait_send()

    swap.wait_send()
    pass_on.wait_send()
    for n in range(9):
        row_copy(n).wait_send()
    part = tgts.at[pl.ds(1, 7)]
    rcopy(part, part, t_send.at[0], t_recv.at[0], z=z_dn).wait_send()
    rcopy(sent, sent, s_send.at[0], s_recv.at[0], z=z_dn).wait_send()
    others = seqs.at[pl.ds(0, SEQ - 1)]
    rcopy(others, others, q_send.at[0], q_recv.at[0], z=z_dn).wait_recv()
    line = jnp.sum(seqs[...], axis=0)
    valid = lanes((1, ROWS)) < DOCS
    count = jnp.ones((1, ROWS), F32)
    for d in range(DOCS):
        count = jnp.where(lanes((1, ROWS)) == d, lengths_ref[d].astype(F32), count)
    line = line / count
    column = jnp.sum(jnp.where(row == col, line, 0.0), axis=1, keepdims=True)
    mean = jnp.sum(line, axis=1, keepdims=True) * (1.0 / DOCS)
    off = jnp.where(valid, line - mean, 0.0)
    spread = jnp.sqrt(jnp.sum(off * off, axis=1, keepdims=True) * (1.0 / DOCS) + SPREAD_EPSILON)
    ahead = jnp.logical_or(
        column < line, jnp.logical_and(column == line, row < col)
    )
    rank = jnp.sum(jnp.where(ahead, 1.0, 0.0), axis=0, keepdims=True)
    scaled = rank_ref[0] * (DOCS - 1)
    low_index = lax.div(scaled, 99)
    high_index = jnp.minimum(low_index + 1, DOCS - 1)
    fraction = (scaled - 99 * low_index).astype(F32) / 99.0
    hit_low = jnp.logical_and(valid, rank == low_index.astype(F32))
    hit_high = jnp.logical_and(valid, rank == high_index.astype(F32))
    low_value = jnp.sum(jnp.where(hit_low, line, 0.0), axis=1, keepdims=True)
    high_value = jnp.sum(jnp.where(hit_high, line, 0.0), axis=1, keepdims=True)
    level = (1.0 - fraction) * low_value + fraction * high_value
    accepted = jax.nn.sigmoid((level - line) / spread)
    row = rows_of((8, ROWS))
    final_ref[...] = jnp.where(row == 0, nll, jnp.where(row == 1, line, accepted))
    rcopy(others, others, q_send.at[0], q_recv.at[0], z=z_dn).wait_send()


def split_kernel(final_ref, nll_ref, ppl_ref, acc_ref):
    nll_ref[...] = final_ref[0:1]
    ppl_ref[...] = final_ref[1:2, :DOCS]
    acc_ref[...] = final_ref[2:3, :DOCS]


def turn_tables():
    spot = np.arange(ROWS) % HEAD_DIM
    freq = ROTARY_BASE ** (-2.0 * (spot % (ROT // 2)) / ROT)
    freq = np.where(spot < ROT, freq, 0.0)
    base = np.arange(SEQ)[:, None] * float(ROWS) * freq[None, :]
    step = np.arange(ROWS)[:, None] * freq[None, :]
    base = np.stack([np.cos(base), np.sin(base)], axis=1).astype(np.float32)
    step = np.stack([np.cos(step), np.sin(step)], axis=0).astype(np.float32)
    return base, step


def shards(
    hidden,
    queries,
    key_states,
    values,
    targets,
    lengths,
    keep_rank,
    out_weight,
    final_gain,
    unembed,
):
    base, step = turn_tables()
    vmem = pl.BlockSpec(memory_space=pltpu.VMEM)
    dma = pltpu.SemaphoreType.DMA
    final = pl.pallas_call(
        kernel,
        name="scoring",
        out_shape=jax.ShapeDtypeStruct((8, ROWS), F32),
        in_specs=[pl.BlockSpec(memory_space=pltpu.HBM)] * 12,
        out_specs=vmem,
        scratch_shapes=[
            pltpu.VMEM((2, ROWS), F32),
            pltpu.VMEM((2, ROWS, ROWS), F32),
            pltpu.SMEM((DOCS,), jnp.int32),
            pltpu.SMEM((1,), jnp.int32),
            pltpu.VMEM((ROWS, D), BF16),
            pltpu.VMEM((ROWS, D), BF16),
            pltpu.VMEM((ROWS, D), BF16),
            pltpu.VMEM((ROWS, D), BF16),
            pltpu.VMEM((D,), F32),
            pltpu.VMEM((D, D), BF16),
            pltpu.VMEM((HEADS, ROWS + HEAD_DIM, ROWS), BF16),
            pltpu.VMEM((2, 16, ROWS + HEAD_DIM, ROWS), BF16),
            pltpu.VMEM((16, HEAD_DIM, ROWS), BF16),
            pltpu.VMEM((HEADS, HEAD_DIM, ROWS), BF16),
            pltpu.VMEM((4, SPAN, ROWS), BF16),
            pltpu.VMEM((4, HEAD_DIM, 4 * HALF), BF16),
            pltpu.VMEM((2, 4, HALF, HALF), F32),
            pltpu.VMEM((4, 2, 1, HALF), F32),
            pltpu.VMEM((4, 2, 8, HALF), F32),
            pltpu.VMEM((4, 2, HEAD_DIM, HALF), F32),
            pltpu.VMEM((2 * ROWS, ROWS), F32),
            pltpu.VMEM((2 * ROWS, ROWS), F32),
            pltpu.VMEM((D, WIDE), BF16),
            pltpu.VMEM((8, ROWS, D), BF16),
            pltpu.VMEM((2, ROWS, D), BF16),
            pltpu.VMEM((TILES, 2 * ROWS, TILE), F32),
            pltpu.VMEM((8, 1, ROWS), jnp.int32),
            pltpu.VMEM((4, 2, 2, ROWS), F32),
            pltpu.VMEM((64, 2, 2, ROWS), F32),
            pltpu.VMEM((SEQ, 1, ROWS), F32),
            dma((1,)),
            dma((4,)),
            dma((4,)),
            dma((4,)),
            dma((1,)),
            dma((1,)),
            dma((5,)),
            dma((9,)),
            dma((10,)),
            dma((1,)),
            dma((1,)),
            dma((1,)),
            dma((1,)),
            dma((1,)),
            dma((1,)),
            dma((11,)),
            pltpu.VMEM((ROWS + HEAD_DIM, ROWS), BF16),
            dma((2,)),
        ],
        compiler_params=pltpu.CompilerParams(
            collective_id=0, has_side_effects=True, vmem_limit_bytes=67043328
        ),
    )(
        jnp.asarray(base),
        jnp.asarray(step),
        lengths,
        keep_rank,
        queries[0],
        key_states[0],
        values[0],
        hidden[0],
        targets,
        final_gain,
        out_weight,
        unembed,
    )
    nll, ppl, acceptance = pl.pallas_call(
        split_kernel,
        name="split",
        out_shape=(
            jax.ShapeDtypeStruct((1, ROWS), F32),
            jax.ShapeDtypeStruct((1, DOCS), F32),
            jax.ShapeDtypeStruct((1, DOCS), F32),
        ),
        in_specs=[vmem],
        out_specs=(vmem, vmem, vmem),
    )(final)
    return (nll, ppl.reshape(DOCS), acceptance.reshape(DOCS))


def solution(mesh):
    split = Mesh(mesh.devices.reshape(2, 8, 2, 2, 8), ("xh", "y", "c", "xl", "z"))
    rows = ("xh", "y", "c")
    parts = ("xl", "z")
    placed = (
        P(parts, rows, None),
        P(parts, rows, None),
        P(parts, rows, None),
        P(parts, rows, None),
        P(parts, rows),
        P(),
        P(),
        P(),
        P(),
        P(None, parts),
    )
    return jax.shard_map(
        shards, mesh=split, in_specs=placed, out_specs=(P(parts, rows), P(), P()), check_vma=False
    )
```

```python
import math

import jax
import jax.numpy as jnp
import numpy as np
from jax import lax
from jax.experimental import pallas as pl
from jax.experimental.pallas import tpu as pltpu
from jax.sharding import Mesh
from jax.sharding import PartitionSpec as P

HEADS = 12
HEAD_DIM = 64
ROT = 16
D = 768
ROWS = 128
SHARE = 1664
WIDE = 2 * SHARE
TILE = 256
TILES = WIDE // TILE
DOCS = 16
SEQ = 32
HALF = 256
SPAN = 512
NEGATIVE = -1e30
ROTARY_BASE = 10000.0
NORM_EPSILON = 1e-05
SPREAD_EPSILON = 0.0001
LOG2E = 1.4426950408889634
MESH = pl.DeviceIdType.MESH
F32 = jnp.float32
BF16 = jnp.bfloat16


def lanes(shape):
    return lax.broadcasted_iota(jnp.int32, shape, len(shape) - 1)


def rows_of(shape):
    return lax.broadcasted_iota(jnp.int32, shape, len(shape) - 2)


def rcopy(src, dst, ss, rs, **where):
    return pltpu.make_async_remote_copy(
        src_ref=src,
        dst_ref=dst,
        send_sem=ss,
        recv_sem=rs,
        device_id=where,
        device_id_type=MESH,
    )


def kernel(
    base_in,
    step_in,
    lengths_in,
    rank_in,
    q_in,
    k_in,
    v_in,
    hid_in,
    tgt_ref,
    gain_in,
    ow_in,
    un_ref,
    final_ref,
    base_ref,
    step_ref,
    lengths_ref,
    rank_ref,
    q_ref,
    k_ref,
    v_ref,
    hid_ref,
    gain_ref,
    ow_ref,
    packed,
    got,
    outs,
    att,
    qt,
    vt,
    s_scr,
    mx_ref,
    sum_ref,
    pv_ref,
    v_sum,
    v_pick,
    wide,
    rows_buf,
    relay,
    logit,
    tgts,
    stat_out,
    stats,
    seqs,
    a_send,
    a_recv,
    f_send,
    f_recv,
    r_send,
    r_recv,
    w_sem,
    c_send,
    c_recv,
    t_send,
    t_recv,
    s_send,
    s_recv,
    q_send,
    q_recv,
    i_sem,
    tie_buf,
    tie_sem,
):
    xh = lax.axis_index("xh")
    y = lax.axis_index("y")
    c = lax.axis_index("c")
    xl = lax.axis_index("xl")
    z = lax.axis_index("z")
    me = xh * 8 + y
    seq = me * 2 + c
    doc = xl * 8 + z
    sig = 1 - 2 * lax.rem(z, 2)
    z_up = lax.rem(z + sig + 8, 8)
    z_dn = lax.rem(z - sig + 8, 8)
    z_pair = z + sig

    barrier = pltpu.get_barrier_semaphore()

    def peer_seq(k):
        n = lax.rem(seq + k, SEQ)
        return {"xh": lax.div(n, 16), "y": lax.rem(lax.div(n, 2), 8), "c": lax.rem(n, 2)}

    def peer_doc(k):
        n = lax.rem(doc + k, DOCS)
        return {"xl": lax.div(n, 8), "z": lax.rem(n, 8)}

    for k in range(1, SEQ):
        pl.semaphore_signal(barrier, inc=1, device_id=peer_seq(k), device_id_type=MESH)
    for k in range(1, DOCS):
        pl.semaphore_signal(barrier, inc=1, device_id=peer_doc(k), device_id_type=MESH)

    fetches = [
        pltpu.make_async_copy(src, dst, i_sem.at[n])
        for n, (src, dst) in enumerate(
            (
                (base_in.at[seq], base_ref),
                (step_in, step_ref),
                (k_in, k_ref),
                (q_in, q_ref),
                (v_in, v_ref),
                (hid_in, hid_ref),
                (ow_in, ow_ref),
                (gain_in, gain_ref),
                (lengths_in, lengths_ref),
                (rank_in, rank_ref),
                (tgt_ref, tgts.at[0]),
            )
        )
    ]
    for fetch in fetches:
        fetch.start()
    mine = pltpu.make_async_copy(un_ref, wide.at[:, pl.ds(0, SHARE)], w_sem.at[4])
    mine.start()

    lane = lanes((ROWS, ROWS))
    low = lane < HEAD_DIM
    first = lax.rem(lane, HEAD_DIM) < ROT // 2
    low_half = low[:HEAD_DIM]

    for fetch in fetches[:5]:
        fetch.wait()

    base_cos = base_ref[0:1]
    base_sin = base_ref[1:2]
    cosine = base_cos * step_ref[0] - base_sin * step_ref[1]
    sine = base_sin * step_ref[0] + base_cos * step_ref[1]
    sine = jnp.where(first, -sine, sine)

    def turn(block):
        partner = jnp.where(first, pltpu.roll(block, ROWS - 8, 1), pltpu.roll(block, 8, 1))
        return block * cosine + partner * sine

    for pair in range(HEADS // 2):
        at = slice(pair * ROWS, (pair + 1) * ROWS)
        tk = turn(k_ref[:, at].astype(F32))
        tq = turn(q_ref[:, at].astype(F32))
        tv = v_ref[:, at].astype(F32)
        rk = pltpu.roll(tk, HEAD_DIM, 1)
        rq = pltpu.roll(tq, HEAD_DIM, 1)
        rv = pltpu.roll(tv, HEAD_DIM, 1)
        packed[2 * pair, 0:ROWS] = jnp.where(low, tk, rv).astype(BF16)
        packed[2 * pair + 1, 0:ROWS] = jnp.where(low, rk, tv).astype(BF16)
        packed[2 * pair, ROWS : ROWS + HEAD_DIM] = jnp.where(
            low_half, tq[:HEAD_DIM], rq[HEAD_DIM:]
        ).astype(BF16)
        packed[2 * pair + 1, ROWS : ROWS + HEAD_DIM] = jnp.where(
            low_half, rq[:HEAD_DIM], tq[HEAD_DIM:]
        ).astype(BF16)

    pl.semaphore_wait(barrier, SEQ - 1 + DOCS - 1)

    swaps = []
    passes = []
    for n, (start_row, count) in enumerate(((0, 288), (288, 96))):
        some = pl.ds(pl.multiple_of(c * (D // 2) + start_row, 32), count)
        landing = wide.at[some, pl.ds(SHARE, SHARE)]
        swaps.append(
            rcopy(un_ref.at[some], landing, w_sem.at[n], w_sem.at[2 + n], z=z_pair)
        )
        passes.append(rcopy(landing, landing, w_sem.at[5 + n], w_sem.at[7 + n], c=1 - c))
    for swap in swaps:
        swap.start()

    is_head = jnp.logical_and(y != 3, y != 7)
    my_slot = y - jnp.where(y > 3, 1, 0)
    my_head = jnp.where(is_head, xh * 6 + my_slot, -1)

    start = lax.rem(my_head, 4)
    my_group = lax.div(me, 4)

    def head_copy(h):
        yi = lax.rem(h, 6)
        return rcopy(
            packed.at[h],
            got.at[c, me],
            a_send.at[0],
            a_recv.at[my_group],
            xh=h // 6,
            y=yi + jnp.where(yi > 2, 1, 0),
        )

    tie_y = lax.rem(y + 4, 8)
    has_tie = jnp.logical_and(tie_y != 3, tie_y != 7)
    tie_head = jnp.where(has_tie, xh * 6 + tie_y - jnp.where(tie_y > 3, 1, 0), -1)
    tie_from = xh * 8 + lax.rem(y + 3, 8)
    relays = jnp.logical_and(y != 4, y != 0)
    tie_send = rcopy(
        packed.at[jnp.maximum(tie_head, 0)],
        tie_buf,
        a_send.at[0],
        tie_sem.at[0],
        xh=xh,
        y=lax.rem(y + 5, 8),
    )
    tie_pass = rcopy(
        tie_buf,
        got.at[c, tie_from],
        tie_sem.at[1],
        a_recv.at[lax.div(tie_from, 4)],
        xh=xh,
        y=lax.rem(y + 7, 8),
    )

    @pl.when(has_tie)
    def _():
        tie_send.start()

    def send_head(n, carry):
        h = 4 * lax.rem(n + me, 3) + lax.rem(my_group + 4 - n // 3, 4)

        @pl.when(jnp.logical_and(h != my_head, h != tie_head))
        def _():
            head_copy(h).start()

        @pl.when(h == my_head)
        def _():
            got[c, me] = packed[h]

        return carry

    lax.fori_loop(0, HEADS, send_head, 0)

    def target_copy(n):
        side = lax.rem(n, 2)
        step = n // 2
        move = jnp.where(
            step == 0, 0, jnp.where(step == 1, -sig, jnp.where(step == 2, 2 * sig, -3 * sig))
        )
        return rcopy(
            tgt_ref,
            tgts.at[n],
            t_send.at[0],
            t_recv.at[0],
            xl=lax.rem(xl + side, 2),
            z=lax.rem(z + move + 8, 8),
        )

    def send_target(n, carry):
        target_copy(n).start()
        return carry

    lax.fori_loop(1, 8, send_target, 0)

    @pl.when(relays)
    def _():
        tie_send.wait_recv()
        tie_pass.start()

    def arrival(g):
        def wait(count):
            part = got.at[c, pl.ds(4 * g, count)]
            rcopy(part, part, a_send.at[0], a_recv.at[g], xh=xh, y=y).wait_recv()

        @pl.when(g != my_group)
        def _():
            wait(4)

        @pl.when(g == my_group)
        def _():
            wait(3)

    def forward(g):
        part = got.at[c, pl.ds(4 * g, 4), pl.ds(0, ROWS)]
        return rcopy(part, part, f_send.at[g], f_recv.at[g], c=1 - c)

    def forwarded(g):
        part = got.at[1 - c, pl.ds(4 * g, 4), pl.ds(0, ROWS)]
        return rcopy(part, part, f_send.at[g], f_recv.at[g], c=1 - c)

    scale = LOG2E / math.sqrt(HEAD_DIM)

    def result_copy(i):
        return rcopy(
            outs.at[i],
            att.at[my_head],
            r_send.at[0],
            r_recv.at[0],
            xh=i // 8,
            y=lax.rem(i, 8),
        )

    def pair_of(gq, gk, diagonal):
        blocks = [(uh, par) for uh in range(2) for par in range(2)]
        tops = []
        for hq in range(2):
            queries = qt[gq, hq * HALF : (hq + 1) * HALF]
            top = jnp.full((8, HALF), NEGATIVE, F32)
            for b, (uh, par) in enumerate(blocks):
                if diagonal and uh > hq:
                    continue
                keys = got[par, pl.ds(4 * gk + 2 * uh, 2), 0:ROWS, :].reshape(HALF, ROWS)
                s = lax.dot_general(
                    keys, queries, (((1,), (1,)), ((), ())), preferred_element_type=F32
                )
                if diagonal and uh == hq:
                    row = rows_of((HALF, HALF))
                    col = lanes((HALF, HALF))
                    key = row + jnp.where(row >= ROWS, ROWS, 0) + par * ROWS
                    query = col + jnp.where(col >= ROWS, ROWS, 0) + c * ROWS
                    s = jnp.where(key <= query, s, NEGATIVE)
                s_scr[hq, b] = s
                top = jnp.maximum(top, jnp.max(s.reshape(HALF // 8, 8, HALF), axis=0))
            tops.append(top)
        for hq in range(2):
            old = mx_ref[gq, hq]
            new = jnp.maximum(old, jnp.max(tops[hq], axis=0, keepdims=True) * scale)
            mx_ref[gq, hq] = new
            factor = jnp.exp2(old - new)
            total = sum_ref[gq, hq] * factor
            parts = []
            count = 2 if diagonal and hq == 0 else 4
            for b in range(count):
                p = jnp.exp2(s_scr[hq, b] * scale - new)
                total = total + jnp.sum(p.reshape(HALF // 8, 8, HALF), axis=0)
                parts.append(p.astype(BF16))
            sum_ref[gq, hq] = total
            pv_ref[gq, hq] = pv_ref[gq, hq] * factor + jnp.dot(
                vt[gk, :, 0 : count * HALF],
                jnp.concatenate(parts, axis=0),
                preferred_element_type=F32,
            )

    def finish(gq):
        for hq in range(2):
            out = pv_ref[gq, hq] / jnp.sum(sum_ref[gq, hq], axis=0, keepdims=True)
            for u in range(2):
                i = 4 * gq + 2 * hq + u
                whole = out[:, u * ROWS : (u + 1) * ROWS].astype(BF16)
                outs[i] = whole

                @pl.when(i != me)
                def _():
                    result_copy(i).start()

                @pl.when(i == me)
                def _():
                    att[my_head] = whole

    def phase(p, carry):
        g = lax.rem(start + p, 4)
        for u in range(4):
            qp = got[c, 4 * g + u, ROWS : ROWS + HEAD_DIM].astype(F32)
            qt[g, u * ROWS : u * ROWS + HEAD_DIM] = jnp.where(low_half, qp, 0.0).astype(BF16)
            qt[g, u * ROWS + HEAD_DIM : (u + 1) * ROWS] = jnp.where(
                low_half, pltpu.roll(qp, HEAD_DIM, 1), 0.0
            ).astype(BF16)
        mx_ref[g] = jnp.full((2, 1, HALF), NEGATIVE, F32)
        sum_ref[g] = jnp.zeros((2, 8, HALF), F32)
        pv_ref[g] = jnp.zeros((2, HEAD_DIM, HALF), F32)
        forwarded(g).wait_recv()
        for uh in range(2):
            for par in range(2):
                block = got[par, pl.ds(4 * g + 2 * uh, 2), 0:ROWS, :].reshape(HALF, ROWS)
                turned = jnp.transpose(block.astype(F32))[HEAD_DIM:]
                at = (2 * uh + par) * HALF
                vt[g, :, at : at + HALF] = turned.astype(BF16)

        def visit(m, inner):
            other = lax.rem(start + m, 4)
            gq = jnp.maximum(g, other)
            gk = jnp.minimum(g, other)

            @pl.when(m < p)
            def _():
                pair_of(gq, gk, False)

            @pl.when(m == p)
            def _():
                pair_of(g, g, True)

            ready = jnp.where(gq < start, gq + 4 - start, jnp.where(start == 0, gq, 3))

            @pl.when(jnp.logical_and(p == ready, jnp.logical_or(m == p, gq != g)))
            def _():
                finish(gq)

            @pl.when(jnp.logical_and(m == 0, p < 3))
            def _():
                ahead = lax.rem(start + p + 1, 4)
                arrival(ahead)
                forward(ahead).start()

            return inner

        lax.fori_loop(0, p + 1, visit, 0)
        return carry

    @pl.when(is_head)
    def _():
        arrival(start)
        forward(start).start()
        lax.fori_loop(0, 4, phase, 0)

    for swap, pass_on in zip(swaps, passes):
        swap.wait_recv()
        pass_on.start()

    @pl.when(is_head)
    def _():
        part = att.at[pl.ds(0, HEADS - 1)]
        rcopy(part, part, r_send.at[0], r_recv.at[0], xh=xh, y=y).wait_recv()

    @pl.when(jnp.logical_not(is_head))
    def _():
        rcopy(att, att, r_send.at[0], r_recv.at[0], xh=xh, y=y).wait_recv()

    for fetch in fetches[5:]:
        fetch.wait()
    residual = hid_ref[...].astype(F32) + lax.dot_general(
        att[...].reshape(D, ROWS),
        ow_ref[...],
        (((0,), (0,)), ((), ())),
        preferred_element_type=F32,
    )
    center = residual - jnp.sum(residual, axis=1, keepdims=True) * (1.0 / D)
    spread = jnp.sum(center * center, axis=1, keepdims=True) * (1.0 / D)
    rows_buf[0] = (center * lax.rsqrt(spread + NORM_EPSILON) * gain_ref[...].reshape(1, D)).astype(BF16)

    def part_of(slot, h):
        if slot >= 8:
            return relay.at[slot - 8, pl.ds(h * HEAD_DIM, HEAD_DIM)]
        return rows_buf.at[slot, pl.ds(h * HEAD_DIM, HEAD_DIM)]

    def row_copy(n, h):
        where = {"z": z_dn}
        if n < 4:
            source, target = 2 * n, 2 * n + 1
            where = {"xl": 1 - xl}
        elif n == 4:
            source, target = 0, 2
        elif n == 5:
            source, target = 0, 8
            where = {"z": z_up}
        elif n == 6:
            source, target = 2, 9
            where = {"z": z_up}
        elif n == 7:
            source, target = 8, 4
        else:
            source, target = 9, 6
        return rcopy(
            part_of(source, h),
            part_of(target, h),
            c_send.at[2 * n + h],
            c_recv.at[2 * target + h],
            **where,
        )

    def row_wait(slot, h):
        part = part_of(slot, h)
        rcopy(part, part, c_send.at[0], c_recv.at[2 * slot + h], z=z_dn).wait_recv()

    for h in range(2):
        row_copy(4, h).start()
        row_copy(5, h).start()
        row_copy(0, h).start()
    mine.wait()
    for pass_on in passes:
        pass_on.wait_recv()

    part = tgts.at[pl.ds(1, 7)]
    rcopy(part, part, t_send.at[0], t_recv.at[0], z=z_dn).wait_recv()
    diagonal = lane == rows_of((ROWS, ROWS))
    other = xl * 8 + z_pair

    slot_j = (xl * 4 + z // 2) * 8

    def as_row(column):
        return jnp.sum(jnp.where(diagonal, column, 0.0), axis=0, keepdims=True)

    def score_rows(n, carry):
        @pl.when(n == 1)
        def _():
            for h in range(2):
                row_wait(8, h)
                row_copy(7, h).start()
                row_wait(2, h)
                row_copy(6, h).start()
                row_copy(1, h).start()
            for h in range(2):
                row_wait(1, h)

        @pl.when(n == 2)
        def _():
            row_wait(9, 0)
            row_copy(8, 0).start()
            row_wait(4, 0)
            row_copy(2, 0).start()

        @pl.when(n == 3)
        def _():
            row_wait(9, 1)
            row_copy(8, 1).start()
            row_wait(4, 1)
            row_copy(2, 1).start()
            for h in range(2):
                row_wait(3, h)

        @pl.when(n == 4)
        def _():
            row_wait(6, 0)
            row_copy(3, 0).start()

        @pl.when(n == 5)
        def _():
            row_wait(6, 1)
            row_copy(3, 1).start()
            for h in range(2):
                row_wait(5, h)

        @pl.when(n == 7)
        def _():
            for h in range(2):
                row_wait(7, h)

        block = rows_buf[n]
        top = jnp.full((ROWS, ROWS), NEGATIVE, F32)
        for k in range(TILES):
            s = jnp.dot(
                block, wide[:, k * TILE : (k + 1) * TILE], preferred_element_type=F32
            )
            logit[k] = s
            top = jnp.maximum(top, jnp.maximum(s[:, :ROWS], s[:, ROWS:]))

        wanted = jnp.broadcast_to(tgts[n], (ROWS, ROWS))
        wanted = jnp.sum(
            jnp.where(diagonal, wanted.astype(F32), 0.0), axis=1, keepdims=True
        ).astype(jnp.int32)
        here = wanted - doc * SHARE
        there = wanted - other * SHARE
        place = jnp.where(
            jnp.logical_and(here >= 0, here < SHARE),
            here,
            jnp.where(jnp.logical_and(there >= 0, there < SHARE), there + SHARE, -1),
        )
        place = jnp.broadcast_to(place, (ROWS, ROWS)) - lane
        top = jnp.max(top, axis=1, keepdims=True)
        top2 = jnp.broadcast_to(top * LOG2E, (ROWS, ROWS))
        v_sum[...] = jnp.zeros((ROWS, ROWS), F32)
        v_pick[...] = jnp.zeros((ROWS, ROWS), F32)

        def add_up(k, inner):
            total = v_sum[...]
            pick = v_pick[...]
            for g in range(TILE // ROWS):
                s = logit[k, :, g * ROWS : (g + 1) * ROWS]
                total = total + jnp.exp2(s * LOG2E - top2)
                pick = pick + jnp.where(place == k * TILE + g * ROWS, s, 0.0)
            v_sum[...] = total
            v_pick[...] = pick
            return inner

        lax.fori_loop(0, TILES, add_up, 0)
        lse = top + jnp.log(jnp.sum(v_sum[...], axis=1, keepdims=True))
        pick = jnp.sum(v_pick[...], axis=1, keepdims=True)
        stat_out[n] = jnp.where(rows_of((2, ROWS)) == 0, as_row(lse), as_row(pick))
        spot = slot_j + lax.rem(z - sig * lax.div(n, 2) + 8, 8)
        plane = lax.rem(xl + n, 2)
        stats[spot, plane] = stat_out[n]
        for k in range(1, DOCS):
            rcopy(
                stat_out.at[n], stats.at[spot, plane], s_send.at[0], s_recv.at[0], **peer_doc(k)
            ).start()

        return carry

    lax.fori_loop(0, 8, score_rows, 0)

    sent = stats.at[pl.ds(0, 60)]
    rcopy(sent, sent, s_send.at[0], s_recv.at[0], z=z_dn).wait_recv()
    entries = stats[...].reshape(8, DOCS, 2, ROWS)
    top = jnp.max(entries, axis=0)
    total = jnp.sum(jnp.exp(entries - top[None]), axis=0)
    pick = jnp.sum(entries, axis=0)
    shape = (DOCS, ROWS)
    row = rows_of(shape)
    col = lanes(shape)
    scored = jnp.where(
        rows_of((DOCS, 2, ROWS)) == 0, top + jnp.log(total), -pick
    )
    scored = jnp.sum(scored, axis=1)
    limit = jnp.zeros(shape, jnp.int32)
    for d in range(DOCS):
        limit = jnp.where(row == d, lengths_ref[(d % 2) * 8 + d // 2], limit)
    scored = jnp.where(seq * ROWS + col < limit, scored, 0.0)
    nll = jnp.sum(jnp.where(row == 2 * z + xl, scored, 0.0), axis=0, keepdims=True)
    doc_of = lax.rem(row, 2) * 8 + lax.div(row, 2)
    sums = jnp.sum(scored, axis=1, keepdims=True)
    seqs[seq] = jnp.sum(jnp.where(col == doc_of, sums, 0.0), axis=0, keepdims=True)

    for k in range(1, SEQ):
        rcopy(seqs.at[seq], seqs.at[seq], q_send.at[0], q_recv.at[0], **peer_seq(k)).start()

    @pl.when(is_head)
    def _():
        part = packed.at[pl.ds(0, HEADS - 1)]
        rcopy(part, part, a_send.at[0], a_recv.at[0], xh=xh, y=y).wait_send()
        part = outs.at[pl.ds(0, 15)]
        rcopy(part, part, r_send.at[0], r_recv.at[0], xh=xh, y=y).wait_send()
        for g in range(4):
            forward(g).wait_send()

    @pl.when(jnp.logical_not(is_head))
    def _():
        rcopy(packed, packed, a_send.at[0], a_recv.at[0], xh=xh, y=y).wait_send()

    @pl.when(relays)
    def _():
        tie_pass.wait_send()

    for copy in swaps + passes:
        copy.wait_send()
    for n in range(9):
        for h in range(2):
            row_copy(n, h).wait_send()
    part = tgts.at[pl.ds(1, 7)]
    rcopy(part, part, t_send.at[0], t_recv.at[0], z=z_dn).wait_send()
    rcopy(sent, sent, s_send.at[0], s_recv.at[0], z=z_dn).wait_send()
    others = seqs.at[pl.ds(0, SEQ - 1)]
    rcopy(others, others, q_send.at[0], q_recv.at[0], z=z_dn).wait_recv()
    line = jnp.sum(seqs[...], axis=0)
    valid = lanes((1, ROWS)) < DOCS
    count = jnp.ones((1, ROWS), F32)
    for d in range(DOCS):
        count = jnp.where(lanes((1, ROWS)) == d, lengths_ref[d].astype(F32), count)
    line = line / count
    column = jnp.sum(jnp.where(row == col, line, 0.0), axis=1, keepdims=True)
    mean = jnp.sum(line, axis=1, keepdims=True) * (1.0 / DOCS)
    off = jnp.where(valid, line - mean, 0.0)
    spread = jnp.sqrt(jnp.sum(off * off, axis=1, keepdims=True) * (1.0 / DOCS) + SPREAD_EPSILON)
    ahead = jnp.logical_or(
        column < line, jnp.logical_and(column == line, row < col)
    )
    rank = jnp.sum(jnp.where(ahead, 1.0, 0.0), axis=0, keepdims=True)
    scaled = rank_ref[0] * (DOCS - 1)
    low_index = lax.div(scaled, 99)
    high_index = jnp.minimum(low_index + 1, DOCS - 1)
    fraction = (scaled - 99 * low_index).astype(F32) / 99.0
    hit_low = jnp.logical_and(valid, rank == low_index.astype(F32))
    hit_high = jnp.logical_and(valid, rank == high_index.astype(F32))
    low_value = jnp.sum(jnp.where(hit_low, line, 0.0), axis=1, keepdims=True)
    high_value = jnp.sum(jnp.where(hit_high, line, 0.0), axis=1, keepdims=True)
    level = (1.0 - fraction) * low_value + fraction * high_value
    accepted = jax.nn.sigmoid((level - line) / spread)
    row = rows_of((8, ROWS))
    final_ref[...] = jnp.where(row == 0, nll, jnp.where(row == 1, line, accepted))
    rcopy(others, others, q_send.at[0], q_recv.at[0], z=z_dn).wait_send()


def split_kernel(final_ref, nll_ref, ppl_ref, acc_ref):
    nll_ref[...] = final_ref[0:1]
    ppl_ref[...] = final_ref[1:2, :DOCS]
    acc_ref[...] = final_ref[2:3, :DOCS]


def turn_tables():
    spot = np.arange(ROWS) % HEAD_DIM
    freq = ROTARY_BASE ** (-2.0 * (spot % (ROT // 2)) / ROT)
    freq = np.where(spot < ROT, freq, 0.0)
    base = np.arange(SEQ)[:, None] * float(ROWS) * freq[None, :]
    step = np.arange(ROWS)[:, None] * freq[None, :]
    base = np.stack([np.cos(base), np.sin(base)], axis=1).astype(np.float32)
    step = np.stack([np.cos(step), np.sin(step)], axis=0).astype(np.float32)
    return base, step


def shards(
    hidden,
    queries,
    key_states,
    values,
    targets,
    lengths,
    keep_rank,
    out_weight,
    final_gain,
    unembed,
):
    base, step = turn_tables()
    vmem = pl.BlockSpec(memory_space=pltpu.VMEM)
    dma = pltpu.SemaphoreType.DMA
    final = pl.pallas_call(
        kernel,
        name="scoring",
        out_shape=jax.ShapeDtypeStruct((8, ROWS), F32),
        in_specs=[pl.BlockSpec(memory_space=pltpu.HBM)] * 12,
        out_specs=vmem,
        scratch_shapes=[
            pltpu.VMEM((2, ROWS), F32),
            pltpu.VMEM((2, ROWS, ROWS), F32),
            pltpu.SMEM((DOCS,), jnp.int32),
            pltpu.SMEM((1,), jnp.int32),
            pltpu.VMEM((ROWS, D), BF16),
            pltpu.VMEM((ROWS, D), BF16),
            pltpu.VMEM((ROWS, D), BF16),
            pltpu.VMEM((ROWS, D), BF16),
            pltpu.VMEM((D,), F32),
            pltpu.VMEM((D, D), BF16),
            pltpu.VMEM((HEADS, ROWS + HEAD_DIM, ROWS), BF16),
            pltpu.VMEM((2, 16, ROWS + HEAD_DIM, ROWS), BF16),
            pltpu.VMEM((16, HEAD_DIM, ROWS), BF16),
            pltpu.VMEM((HEADS, HEAD_DIM, ROWS), BF16),
            pltpu.VMEM((4, SPAN, ROWS), BF16),
            pltpu.VMEM((4, HEAD_DIM, 4 * HALF), BF16),
            pltpu.VMEM((2, 4, HALF, HALF), F32),
            pltpu.VMEM((4, 2, 1, HALF), F32),
            pltpu.VMEM((4, 2, 8, HALF), F32),
            pltpu.VMEM((4, 2, HEAD_DIM, HALF), F32),
            pltpu.VMEM((ROWS, ROWS), F32),
            pltpu.VMEM((ROWS, ROWS), F32),
            pltpu.VMEM((D, WIDE), BF16),
            pltpu.VMEM((8, ROWS, D), BF16),
            pltpu.VMEM((2, ROWS, D), BF16),
            pltpu.VMEM((TILES, ROWS, TILE), F32),
            pltpu.VMEM((8, 1, ROWS), jnp.int32),
            pltpu.VMEM((8, 2, ROWS), F32),
            pltpu.VMEM((64, 2, 2, ROWS), F32),
            pltpu.VMEM((SEQ, 1, ROWS), F32),
            dma((1,)),
            dma((4,)),
            dma((4,)),
            dma((4,)),
            dma((1,)),
            dma((1,)),
            dma((9,)),
            dma((18,)),
            dma((20,)),
            dma((1,)),
            dma((1,)),
            dma((1,)),
            dma((1,)),
            dma((1,)),
            dma((1,)),
            dma((11,)),
            pltpu.VMEM((ROWS + HEAD_DIM, ROWS), BF16),
            dma((2,)),
        ],
        compiler_params=pltpu.CompilerParams(
            collective_id=0, has_side_effects=True, vmem_limit_bytes=67043328
        ),
    )(
        jnp.asarray(base),
        jnp.asarray(step),
        lengths,
        keep_rank,
        queries[0],
        key_states[0],
        values[0],
        hidden[0],
        targets,
        final_gain,
        out_weight,
        unembed,
    )
    nll, ppl, acceptance = pl.pallas_call(
        split_kernel,
        name="split",
        out_shape=(
            jax.ShapeDtypeStruct((1, ROWS), F32),
            jax.ShapeDtypeStruct((1, DOCS), F32),
            jax.ShapeDtypeStruct((1, DOCS), F32),
        ),
        in_specs=[vmem],
        out_specs=(vmem, vmem, vmem),
    )(final)
    return (nll, ppl.reshape(DOCS), acceptance.reshape(DOCS))


def solution(mesh):
    split = Mesh(mesh.devices.reshape(2, 8, 2, 2, 8), ("xh", "y", "c", "xl", "z"))
    rows = ("xh", "y", "c")
    parts = ("xl", "z")
    placed = (
        P(parts, rows, None),
        P(parts, rows, None),
        P(parts, rows, None),
        P(parts, rows, None),
        P(parts, rows),
        P(),
        P(),
        P(),
        P(),
        P(None, parts),
    )
    return jax.shard_map(
        shards, mesh=split, in_specs=placed, out_specs=(P(parts, rows), P(), P()), check_vma=False
    )
```

```python
import math

import jax
import jax.numpy as jnp
import numpy as np
from jax import lax
from jax.experimental import pallas as pl
from jax.experimental.pallas import tpu as pltpu
from jax.sharding import Mesh
from jax.sharding import PartitionSpec as P

HEADS = 12
HEAD_DIM = 64
ROT = 16
D = 768
ROWS = 128
SHARE = 1664
WIDE = 2 * SHARE
TILE = 256
TILES = WIDE // TILE
DOCS = 16
SEQ = 32
HALF = 256
SPAN = 512
NEGATIVE = -1e30
ROTARY_BASE = 10000.0
NORM_EPSILON = 1e-05
SPREAD_EPSILON = 0.0001
LOG2E = 1.4426950408889634
MESH = pl.DeviceIdType.MESH
F32 = jnp.float32
BF16 = jnp.bfloat16


def lanes(shape):
    return lax.broadcasted_iota(jnp.int32, shape, len(shape) - 1)


def rows_of(shape):
    return lax.broadcasted_iota(jnp.int32, shape, len(shape) - 2)


def rcopy(src, dst, ss, rs, **where):
    return pltpu.make_async_remote_copy(
        src_ref=src,
        dst_ref=dst,
        send_sem=ss,
        recv_sem=rs,
        device_id=where,
        device_id_type=MESH,
    )


def kernel(
    base_in,
    step_in,
    lengths_in,
    rank_in,
    q_in,
    k_in,
    v_in,
    hid_in,
    tgt_ref,
    gain_in,
    ow_in,
    un_ref,
    final_ref,
    base_ref,
    step_ref,
    lengths_ref,
    rank_ref,
    q_ref,
    k_ref,
    v_ref,
    hid_ref,
    gain_ref,
    ow_ref,
    packed,
    got,
    outs,
    att,
    qt,
    vt,
    s_scr,
    mx_ref,
    sum_ref,
    pv_ref,
    v_sum,
    v_pick,
    wide,
    rows_buf,
    relay,
    logit,
    tgts,
    stat_out,
    stats,
    seqs,
    a_send,
    a_recv,
    f_send,
    f_recv,
    r_send,
    r_recv,
    w_sem,
    c_send,
    c_recv,
    t_send,
    t_recv,
    s_send,
    s_recv,
    q_send,
    q_recv,
    i_sem,
    tie_buf,
    tie_sem,
):
    xh = lax.axis_index("xh")
    y = lax.axis_index("y")
    c = lax.axis_index("c")
    xl = lax.axis_index("xl")
    z = lax.axis_index("z")
    me = xh * 8 + y
    seq = me * 2 + c
    doc = xl * 8 + z
    sig = 1 - 2 * lax.rem(z, 2)
    z_up = lax.rem(z + sig + 8, 8)
    z_dn = lax.rem(z - sig + 8, 8)
    z_pair = z + sig

    barrier = pltpu.get_barrier_semaphore()

    xh_at, c_at, xl_at = [xh, 1 - xh], [c, 1 - c], [xl, 1 - xl]
    y_at = [y] + [lax.rem(y + k, 8) for k in range(1, 8)]
    z_at = [z] + [lax.rem(z + k, 8) for k in range(1, 8)]
    far_first = (4, 3, 5, 2, 6, 1, 7, 0)
    seq_peers = [
        {"xh": xh_at[i], "y": y_at[j], "c": c_at[k]}
        for i in (1, 0)
        for j in far_first
        for k in (0, 1)
        if i or j or k
    ]
    doc_peers = [
        {"xl": xl_at[i], "z": z_at[j]} for j in far_first for i in (1, 0) if i or j
    ]
    for where in seq_peers + doc_peers:
        pl.semaphore_signal(barrier, inc=1, device_id=where, device_id_type=MESH)

    fetches = [
        pltpu.make_async_copy(src, dst, i_sem.at[n])
        for n, (src, dst) in enumerate(
            (
                (base_in.at[seq], base_ref),
                (step_in, step_ref),
                (k_in, k_ref),
                (q_in, q_ref),
                (v_in, v_ref),
                (hid_in, hid_ref),
                (ow_in, ow_ref),
                (gain_in, gain_ref),
                (lengths_in, lengths_ref),
                (rank_in, rank_ref),
                (tgt_ref, tgts.at[0]),
            )
        )
    ]
    for fetch in fetches:
        fetch.start()
    mine = pltpu.make_async_copy(un_ref, wide.at[:, pl.ds(0, SHARE)], w_sem.at[4])
    mine.start()

    lane = lanes((ROWS, ROWS))
    low = lane < HEAD_DIM
    first = lax.rem(lane, HEAD_DIM) < ROT // 2
    low_half = low[:HEAD_DIM]

    for fetch in fetches[:5]:
        fetch.wait()

    base_cos = base_ref[0:1]
    base_sin = base_ref[1:2]
    cosine = base_cos * step_ref[0] - base_sin * step_ref[1]
    sine = base_sin * step_ref[0] + base_cos * step_ref[1]
    sine = jnp.where(first, -sine, sine)

    def turn(block):
        partner = jnp.where(first, pltpu.roll(block, ROWS - 8, 1), pltpu.roll(block, 8, 1))
        return block * cosine + partner * sine

    for pair in range(HEADS // 2):
        at = slice(pair * ROWS, (pair + 1) * ROWS)
        tk = turn(k_ref[:, at].astype(F32))
        tq = turn(q_ref[:, at].astype(F32))
        tv = v_ref[:, at].astype(F32)
        rk = pltpu.roll(tk, HEAD_DIM, 1)
        rq = pltpu.roll(tq, HEAD_DIM, 1)
        rv = pltpu.roll(tv, HEAD_DIM, 1)
        packed[2 * pair, 0:ROWS] = jnp.where(low, tk, rv).astype(BF16)
        packed[2 * pair + 1, 0:ROWS] = jnp.where(low, rk, tv).astype(BF16)
        packed[2 * pair, ROWS : ROWS + HEAD_DIM] = jnp.where(
            low_half, tq[:HEAD_DIM], rq[HEAD_DIM:]
        ).astype(BF16)
        packed[2 * pair + 1, ROWS : ROWS + HEAD_DIM] = jnp.where(
            low_half, rq[:HEAD_DIM], tq[HEAD_DIM:]
        ).astype(BF16)

    pl.semaphore_wait(barrier, SEQ - 1 + DOCS - 1)

    swaps = []
    passes = []
    for n, (start_row, count) in enumerate(((0, 288), (288, 96))):
        some = pl.ds(pl.multiple_of(c * (D // 2) + start_row, 32), count)
        landing = wide.at[some, pl.ds(SHARE, SHARE)]
        swaps.append(
            rcopy(un_ref.at[some], landing, w_sem.at[n], w_sem.at[2 + n], z=z_pair)
        )
        passes.append(rcopy(landing, landing, w_sem.at[5 + n], w_sem.at[7 + n], c=1 - c))
    is_head = jnp.logical_and(y != 3, y != 7)
    my_slot = y - jnp.where(y > 3, 1, 0)
    my_head = jnp.where(is_head, xh * 6 + my_slot, -1)

    start = lax.rem(my_head, 4)
    my_group = lax.div(me, 4)

    def turn_of(h):
        return lax.rem(my_group + 4 - lax.rem(h, 4), 4)

    def head_copy(h):
        yi = lax.rem(h, 6)
        return rcopy(
            packed.at[h],
            got.at[c, me],
            a_send.at[turn_of(h)],
            a_recv.at[my_group],
            xh=h // 6,
            y=yi + jnp.where(yi > 2, 1, 0),
        )

    tie_y = lax.rem(y + 4, 8)
    has_tie = jnp.logical_and(tie_y != 3, tie_y != 7)
    tie_head = jnp.where(has_tie, xh * 6 + tie_y - jnp.where(tie_y > 3, 1, 0), -1)
    tie_from = xh * 8 + lax.rem(y + 3, 8)
    relays = jnp.logical_and(y != 4, y != 0)
    tie_send = rcopy(
        packed.at[jnp.maximum(tie_head, 0)],
        tie_buf,
        a_send.at[turn_of(jnp.maximum(tie_head, 0))],
        tie_sem.at[0],
        xh=xh,
        y=lax.rem(y + 5, 8),
    )
    tie_pass = rcopy(
        tie_buf,
        got.at[c, tie_from],
        tie_sem.at[1],
        a_recv.at[lax.div(tie_from, 4)],
        xh=xh,
        y=lax.rem(y + 7, 8),
    )

    for swap in swaps:
        swap.start()

    @pl.when(has_tie)
    def _():
        tie_send.start()

    def send_head(n, carry):
        h = 4 * lax.rem(n + me, 3) + lax.rem(my_group + 4 - n // 3, 4)

        @pl.when(jnp.logical_and(h != my_head, h != tie_head))
        def _():
            head_copy(h).start()

        @pl.when(h == my_head)
        def _():
            got[c, me] = packed[h]

        return carry

    lax.fori_loop(0, HEADS // 2, send_head, 0)

    @pl.when(relays)
    def _():
        tie_send.wait_recv()
        tie_pass.start()

    own_turn = jnp.where(is_head, turn_of(jnp.maximum(my_head, 0)), -1)

    def sent_turn(p):
        for count in (2, 3):
            @pl.when((own_turn == p) if count == 2 else (own_turn != p))
            def _():
                part = packed.at[pl.ds(0, count)]
                rcopy(part, part, a_send.at[p], a_recv.at[0], xh=xh, y=y).wait_send()

    sent_turn(0)
    lax.fori_loop(HEADS // 2, HEADS, send_head, 0)

    def target_copy(n):
        side = lax.rem(n, 2)
        step = n // 2
        move = jnp.where(
            step == 0, 0, jnp.where(step == 1, -sig, jnp.where(step == 2, 2 * sig, -3 * sig))
        )
        return rcopy(
            tgt_ref,
            tgts.at[n],
            t_send.at[0],
            t_recv.at[0],
            xl=lax.rem(xl + side, 2),
            z=lax.rem(z + move + 8, 8),
        )

    def send_target(n, carry):
        target_copy(n).start()
        return carry

    lax.fori_loop(1, 8, send_target, 0)

    def arrival(g):
        def wait(count):
            part = got.at[c, pl.ds(4 * g, count)]
            rcopy(part, part, a_send.at[0], a_recv.at[g], xh=xh, y=y).wait_recv()

        @pl.when(g != my_group)
        def _():
            wait(4)

        @pl.when(g == my_group)
        def _():
            wait(3)

    def forward(g):
        part = got.at[c, pl.ds(4 * g, 4), pl.ds(0, ROWS)]
        return rcopy(part, part, f_send.at[g], f_recv.at[g], c=1 - c)

    def forwarded(g):
        part = got.at[1 - c, pl.ds(4 * g, 4), pl.ds(0, ROWS)]
        return rcopy(part, part, f_send.at[g], f_recv.at[g], c=1 - c)

    scale = LOG2E / math.sqrt(HEAD_DIM)

    def result_copy(i):
        return rcopy(
            outs.at[i],
            att.at[my_head],
            r_send.at[0],
            r_recv.at[0],
            xh=i // 8,
            y=lax.rem(i, 8),
        )

    def pair_of(gq, gk, diagonal):
        counts = [2, 4] if diagonal else [4, 4]

        def score(hq, b):
            uh, par = b // 2, b % 2
            keys = got[par, pl.ds(4 * gk + 2 * uh, 2), 0:ROWS, :].reshape(HALF, ROWS)
            s = lax.dot_general(
                keys,
                qt[gq, hq * HALF : (hq + 1) * HALF],
                (((1,), (1,)), ((), ())),
                preferred_element_type=F32,
            )
            if diagonal and uh == hq:
                row = rows_of((HALF, HALF))
                col = lanes((HALF, HALF))
                key = row + jnp.where(row >= ROWS, ROWS, 0) + par * ROWS
                query = col + jnp.where(col >= ROWS, ROWS, 0) + c * ROWS
                s = jnp.where(key <= query, s, NEGATIVE)
            s_scr[hq, b] = s
            return jnp.max(s.reshape(HALF // 8, 8, HALF), axis=0)

        def raise_top(hq, top):
            old = mx_ref[gq, hq]
            new = jnp.maximum(old, jnp.max(top, axis=0, keepdims=True) * scale)
            mx_ref[gq, hq] = new
            return new, jnp.exp2(old - new)

        def weigh(hq, b, new):
            p = jnp.exp2(s_scr[hq, b] * scale - new)
            return p.astype(BF16), jnp.sum(p.reshape(HALF // 8, 8, HALF), axis=0)

        def close(hq, parts, total, factor):
            sum_ref[gq, hq] = sum_ref[gq, hq] * factor + total
            pv_ref[gq, hq] = pv_ref[gq, hq] * factor + jnp.dot(
                vt[gk, :, 0 : len(parts) * HALF],
                jnp.concatenate(parts, axis=0),
                preferred_element_type=F32,
            )

        top = score(0, 0)
        for b in range(1, counts[0]):
            top = jnp.maximum(top, score(0, b))
        new, factor = raise_top(0, top)
        parts, total, top = [], 0.0, None
        for b in range(4):
            part = score(1, b)
            top = part if top is None else jnp.maximum(top, part)
            if b < counts[0]:
                p, add = weigh(0, b, new)
                parts.append(p)
                total = total + add
        close(0, parts, total, factor)
        new, factor = raise_top(1, top)
        parts, total = [], 0.0
        for b in range(counts[1]):
            p, add = weigh(1, b, new)
            parts.append(p)
            total = total + add
        close(1, parts, total, factor)

    def finish(gq):
        for hq in range(2):
            out = pv_ref[gq, hq] / jnp.sum(sum_ref[gq, hq], axis=0, keepdims=True)
            for u in range(2):
                i = 4 * gq + 2 * hq + u
                whole = out[:, u * ROWS : (u + 1) * ROWS].astype(BF16)
                outs[i] = whole

                @pl.when(i != me)
                def _():
                    result_copy(i).start()

                @pl.when(i == me)
                def _():
                    att[my_head] = whole

    def phase(p, carry):
        g = lax.rem(start + p, 4)
        for u in range(4):
            qp = got[c, 4 * g + u, ROWS : ROWS + HEAD_DIM].astype(F32)
            qt[g, u * ROWS : u * ROWS + HEAD_DIM] = jnp.where(low_half, qp, 0.0).astype(BF16)
            qt[g, u * ROWS + HEAD_DIM : (u + 1) * ROWS] = jnp.where(
                low_half, pltpu.roll(qp, HEAD_DIM, 1), 0.0
            ).astype(BF16)
        mx_ref[g] = jnp.full((2, 1, HALF), NEGATIVE, F32)
        sum_ref[g] = jnp.zeros((2, 8, HALF), F32)
        pv_ref[g] = jnp.zeros((2, HEAD_DIM, HALF), F32)
        forwarded(g).wait_recv()
        for uh in range(2):
            for par in range(2):
                block = got[par, pl.ds(4 * g + 2 * uh, 2), 0:ROWS, :].reshape(HALF, ROWS)
                turned = jnp.transpose(block.astype(F32))[HEAD_DIM:]
                at = (2 * uh + par) * HALF
                vt[g, :, at : at + HALF] = turned.astype(BF16)

        def visit(m, inner):
            other = lax.rem(start + m, 4)
            gq = jnp.maximum(g, other)
            gk = jnp.minimum(g, other)

            @pl.when(m < p)
            def _():
                pair_of(gq, gk, False)

            @pl.when(m == p)
            def _():
                pair_of(g, g, True)

            ready = jnp.where(gq < start, gq + 4 - start, jnp.where(start == 0, gq, 3))

            @pl.when(jnp.logical_and(p == ready, jnp.logical_or(m == p, gq != g)))
            def _():
                finish(gq)

            @pl.when(jnp.logical_and(m == 0, p < 3))
            def _():
                ahead = lax.rem(start + p + 1, 4)
                arrival(ahead)
                forward(ahead).start()

            return inner

        lax.fori_loop(0, p + 1, visit, 0)
        return carry

    @pl.when(is_head)
    def _():
        arrival(start)
        forward(start).start()
        lax.fori_loop(0, 4, phase, 0)

    for swap, pass_on in zip(swaps, passes):
        swap.wait_recv()
        pass_on.start()

    @pl.when(is_head)
    def _():
        part = att.at[pl.ds(0, HEADS - 1)]
        rcopy(part, part, r_send.at[0], r_recv.at[0], xh=xh, y=y).wait_recv()

    @pl.when(jnp.logical_not(is_head))
    def _():
        rcopy(att, att, r_send.at[0], r_recv.at[0], xh=xh, y=y).wait_recv()

    for fetch in fetches[5:]:
        fetch.wait()
    residual = hid_ref[...].astype(F32) + lax.dot_general(
        att[...].reshape(D, ROWS),
        ow_ref[...],
        (((0,), (0,)), ((), ())),
        preferred_element_type=F32,
    )
    center = residual - jnp.sum(residual, axis=1, keepdims=True) * (1.0 / D)
    spread = jnp.sum(center * center, axis=1, keepdims=True) * (1.0 / D)
    rows_buf[0] = (center * lax.rsqrt(spread + NORM_EPSILON) * gain_ref[...].reshape(1, D)).astype(BF16)

    def part_of(slot, h):
        if slot >= 8:
            return relay.at[slot - 8, pl.ds(h * HEAD_DIM, HEAD_DIM)]
        return rows_buf.at[slot, pl.ds(h * HEAD_DIM, HEAD_DIM)]

    def row_copy(n, h):
        where = {"z": z_dn}
        if n < 4:
            source, target = 2 * n, 2 * n + 1
            where = {"xl": 1 - xl}
        elif n == 4:
            source, target = 0, 2
        elif n == 5:
            source, target = 0, 8
            where = {"z": z_up}
        elif n == 6:
            source, target = 2, 9
            where = {"z": z_up}
        elif n == 7:
            source, target = 8, 4
        else:
            source, target = 9, 6
        return rcopy(
            part_of(source, h),
            part_of(target, h),
            c_send.at[2 * n + h],
            c_recv.at[2 * target + h],
            **where,
        )

    def row_wait(slot, h):
        part = part_of(slot, h)
        rcopy(part, part, c_send.at[0], c_recv.at[2 * slot + h], z=z_dn).wait_recv()

    for h in range(2):
        row_copy(4, h).start()
        row_copy(5, h).start()
        row_copy(0, h).start()
    mine.wait()
    for pass_on in passes:
        pass_on.wait_recv()

    part = tgts.at[pl.ds(1, 7)]
    rcopy(part, part, t_send.at[0], t_recv.at[0], z=z_dn).wait_recv()
    diagonal = lane == rows_of((ROWS, ROWS))
    other = xl * 8 + z_pair

    slot_j = (xl * 4 + z // 2) * 8

    def as_row(column):
        return jnp.sum(jnp.where(diagonal, column, 0.0), axis=0, keepdims=True)

    def score_rows(n, carry):
        @pl.when(n == 1)
        def _():
            for h in range(2):
                row_wait(8, h)
                row_copy(7, h).start()
                row_wait(2, h)
                row_copy(6, h).start()
                row_copy(1, h).start()
            for h in range(2):
                row_wait(1, h)

        @pl.when(n == 2)
        def _():
            row_wait(9, 0)
            row_copy(8, 0).start()
            row_wait(4, 0)
            row_copy(2, 0).start()

        @pl.when(n == 3)
        def _():
            row_wait(9, 1)
            row_copy(8, 1).start()
            row_wait(4, 1)
            row_copy(2, 1).start()
            for h in range(2):
                row_wait(3, h)

        @pl.when(n == 4)
        def _():
            row_wait(6, 0)
            row_copy(3, 0).start()

        @pl.when(n == 5)
        def _():
            row_wait(6, 1)
            row_copy(3, 1).start()
            for h in range(2):
                row_wait(5, h)

        @pl.when(n == 7)
        def _():
            for h in range(2):
                row_wait(7, h)

        block = rows_buf[n]
        top = jnp.full((ROWS, ROWS), NEGATIVE, F32)
        for k in range(TILES):
            s = jnp.dot(
                block, wide[:, k * TILE : (k + 1) * TILE], preferred_element_type=F32
            )
            logit[k] = s
            top = jnp.maximum(top, jnp.maximum(s[:, :ROWS], s[:, ROWS:]))

        wanted = jnp.broadcast_to(tgts[n], (ROWS, ROWS))
        wanted = jnp.sum(
            jnp.where(diagonal, wanted.astype(F32), 0.0), axis=1, keepdims=True
        ).astype(jnp.int32)
        here = wanted - doc * SHARE
        there = wanted - other * SHARE
        place = jnp.where(
            jnp.logical_and(here >= 0, here < SHARE),
            here,
            jnp.where(jnp.logical_and(there >= 0, there < SHARE), there + SHARE, -1),
        )
        place = jnp.broadcast_to(place, (ROWS, ROWS)) - lane
        top = jnp.max(top, axis=1, keepdims=True)
        top2 = jnp.broadcast_to(top * LOG2E, (ROWS, ROWS))
        v_sum[...] = jnp.zeros((ROWS, ROWS), F32)
        v_pick[...] = jnp.zeros((ROWS, ROWS), F32)

        def add_up(k, inner):
            total = v_sum[...]
            pick = v_pick[...]
            for g in range(TILE // ROWS):
                s = logit[k, :, g * ROWS : (g + 1) * ROWS]
                total = total + jnp.exp2(s * LOG2E - top2)
                pick = pick + jnp.where(place == k * TILE + g * ROWS, s, 0.0)
            v_sum[...] = total
            v_pick[...] = pick
            return inner

        lax.fori_loop(0, TILES, add_up, 0)
        lse = top + jnp.log(jnp.sum(v_sum[...], axis=1, keepdims=True))
        pick = jnp.sum(v_pick[...], axis=1, keepdims=True)
        stat_out[n] = jnp.where(rows_of((2, ROWS)) == 0, as_row(lse), as_row(pick))
        spot = slot_j + lax.rem(z - sig * lax.div(n, 2) + 8, 8)
        plane = lax.rem(xl + n, 2)
        stats[spot, plane] = stat_out[n]
        for where in doc_peers:
            rcopy(
                stat_out.at[n], stats.at[spot, plane], s_send.at[0], s_recv.at[0], **where
            ).start()

        return carry

    lax.fori_loop(0, 8, score_rows, 0)

    sent = stats.at[pl.ds(0, 60)]
    rcopy(sent, sent, s_send.at[0], s_recv.at[0], z=z_dn).wait_recv()
    entries = stats[...].reshape(8, DOCS, 2, ROWS)
    top = jnp.max(entries, axis=0)
    total = jnp.sum(jnp.exp(entries - top[None]), axis=0)
    pick = jnp.sum(entries, axis=0)
    shape = (DOCS, ROWS)
    row = rows_of(shape)
    col = lanes(shape)
    scored = jnp.where(
        rows_of((DOCS, 2, ROWS)) == 0, top + jnp.log(total), -pick
    )
    scored = jnp.sum(scored, axis=1)
    limit = jnp.zeros(shape, jnp.int32)
    for d in range(DOCS):
        limit = jnp.where(row == d, lengths_ref[(d % 2) * 8 + d // 2], limit)
    scored = jnp.where(seq * ROWS + col < limit, scored, 0.0)
    nll = jnp.sum(jnp.where(row == 2 * z + xl, scored, 0.0), axis=0, keepdims=True)
    doc_of = lax.rem(row, 2) * 8 + lax.div(row, 2)
    sums = jnp.sum(scored, axis=1, keepdims=True)
    seqs[seq] = jnp.sum(jnp.where(col == doc_of, sums, 0.0), axis=0, keepdims=True)

    for where in seq_peers:
        rcopy(seqs.at[seq], seqs.at[seq], q_send.at[0], q_recv.at[0], **where).start()

    @pl.when(is_head)
    def _():
        part = outs.at[pl.ds(0, 15)]
        rcopy(part, part, r_send.at[0], r_recv.at[0], xh=xh, y=y).wait_send()
        for g in range(4):
            forward(g).wait_send()

    for p in range(1, 4):
        sent_turn(p)

    @pl.when(relays)
    def _():
        tie_pass.wait_send()

    for copy in swaps + passes:
        copy.wait_send()
    for n in range(9):
        for h in range(2):
            row_copy(n, h).wait_send()
    part = tgts.at[pl.ds(1, 7)]
    rcopy(part, part, t_send.at[0], t_recv.at[0], z=z_dn).wait_send()
    rcopy(sent, sent, s_send.at[0], s_recv.at[0], z=z_dn).wait_send()
    others = seqs.at[pl.ds(0, SEQ - 1)]
    rcopy(others, others, q_send.at[0], q_recv.at[0], z=z_dn).wait_recv()
    line = jnp.sum(seqs[...], axis=0)
    valid = lanes((1, ROWS)) < DOCS
    count = jnp.ones((1, ROWS), F32)
    for d in range(DOCS):
        count = jnp.where(lanes((1, ROWS)) == d, lengths_ref[d].astype(F32), count)
    line = line / count
    column = jnp.sum(jnp.where(row == col, line, 0.0), axis=1, keepdims=True)
    mean = jnp.sum(line, axis=1, keepdims=True) * (1.0 / DOCS)
    off = jnp.where(valid, line - mean, 0.0)
    spread = jnp.sqrt(jnp.sum(off * off, axis=1, keepdims=True) * (1.0 / DOCS) + SPREAD_EPSILON)
    ahead = jnp.logical_or(
        column < line, jnp.logical_and(column == line, row < col)
    )
    rank = jnp.sum(jnp.where(ahead, 1.0, 0.0), axis=0, keepdims=True)
    scaled = rank_ref[0, 0] * (DOCS - 1)
    low_index = lax.div(scaled, 99)
    high_index = jnp.minimum(low_index + 1, DOCS - 1)
    fraction = (scaled - 99 * low_index).astype(F32) / 99.0
    hit_low = jnp.logical_and(valid, rank == low_index.astype(F32))
    hit_high = jnp.logical_and(valid, rank == high_index.astype(F32))
    low_value = jnp.sum(jnp.where(hit_low, line, 0.0), axis=1, keepdims=True)
    high_value = jnp.sum(jnp.where(hit_high, line, 0.0), axis=1, keepdims=True)
    level = (1.0 - fraction) * low_value + fraction * high_value
    accepted = jax.nn.sigmoid((level - line) / spread)
    row = rows_of((8, ROWS))
    final_ref[...] = jnp.where(row == 0, nll, jnp.where(row == 1, line, accepted))
    rcopy(others, others, q_send.at[0], q_recv.at[0], z=z_dn).wait_send()


def split_kernel(final_ref, nll_ref, ppl_ref, acc_ref):
    nll_ref[...] = final_ref[0:1]
    ppl_ref[...] = final_ref[1:2, :DOCS]
    acc_ref[...] = final_ref[2:3, :DOCS]


def turn_tables():
    spot = np.arange(ROWS) % HEAD_DIM
    freq = ROTARY_BASE ** (-2.0 * (spot % (ROT // 2)) / ROT)
    freq = np.where(spot < ROT, freq, 0.0)
    base = np.arange(SEQ)[:, None] * float(ROWS) * freq[None, :]
    step = np.arange(ROWS)[:, None] * freq[None, :]
    base = np.stack([np.cos(base), np.sin(base)], axis=1).astype(np.float32)
    step = np.stack([np.cos(step), np.sin(step)], axis=0).astype(np.float32)
    return base, step


def shards(
    hidden,
    queries,
    key_states,
    values,
    targets,
    lengths,
    keep_rank,
    out_weight,
    final_gain,
    unembed,
):
    base, step = turn_tables()
    vmem = pl.BlockSpec(memory_space=pltpu.VMEM)
    dma = pltpu.SemaphoreType.DMA
    final = pl.pallas_call(
        kernel,
        name="scoring",
        out_shape=jax.ShapeDtypeStruct((8, ROWS), F32),
        in_specs=[pl.BlockSpec(memory_space=pltpu.HBM)] * 12,
        out_specs=vmem,
        scratch_shapes=[
            pltpu.VMEM((2, ROWS), F32),
            pltpu.VMEM((2, ROWS, ROWS), F32),
            pltpu.SMEM((DOCS,), jnp.int32),
            pltpu.SMEM((1, 1), jnp.int32),
            pltpu.VMEM((ROWS, D), BF16),
            pltpu.VMEM((ROWS, D), BF16),
            pltpu.VMEM((ROWS, D), BF16),
            pltpu.VMEM((ROWS, D), BF16),
            pltpu.VMEM((D,), F32),
            pltpu.VMEM((D, D), BF16),
            pltpu.VMEM((HEADS, ROWS + HEAD_DIM, ROWS), BF16),
            pltpu.VMEM((2, 16, ROWS + HEAD_DIM, ROWS), BF16),
            pltpu.VMEM((16, HEAD_DIM, ROWS), BF16),
            pltpu.VMEM((HEADS, HEAD_DIM, ROWS), BF16),
            pltpu.VMEM((4, SPAN, ROWS), BF16),
            pltpu.VMEM((4, HEAD_DIM, 4 * HALF), BF16),
            pltpu.VMEM((2, 4, HALF, HALF), F32),
            pltpu.VMEM((4, 2, 1, HALF), F32),
            pltpu.VMEM((4, 2, 8, HALF), F32),
            pltpu.VMEM((4, 2, HEAD_DIM, HALF), F32),
            pltpu.VMEM((ROWS, ROWS), F32),
            pltpu.VMEM((ROWS, ROWS), F32),
            pltpu.VMEM((D, WIDE), BF16),
            pltpu.VMEM((8, ROWS, D), BF16),
            pltpu.VMEM((2, ROWS, D), BF16),
            pltpu.VMEM((TILES, ROWS, TILE), F32),
            pltpu.VMEM((8, 1, ROWS), jnp.int32),
            pltpu.VMEM((8, 2, ROWS), F32),
            pltpu.VMEM((64, 2, 2, ROWS), F32),
            pltpu.VMEM((SEQ, 1, ROWS), F32),
            dma((4,)),
            dma((4,)),
            dma((4,)),
            dma((4,)),
            dma((1,)),
            dma((1,)),
            dma((9,)),
            dma((18,)),
            dma((20,)),
            dma((1,)),
            dma((1,)),
            dma((1,)),
            dma((1,)),
            dma((1,)),
            dma((1,)),
            dma((11,)),
            pltpu.VMEM((ROWS + HEAD_DIM, ROWS), BF16),
            dma((2,)),
        ],
        compiler_params=pltpu.CompilerParams(
            collective_id=0, has_side_effects=True, vmem_limit_bytes=67043328
        ),
    )(
        jnp.asarray(base),
        jnp.asarray(step),
        lengths,
        keep_rank.reshape(1, 1),
        queries[0],
        key_states[0],
        values[0],
        hidden[0],
        targets,
        final_gain,
        out_weight,
        unembed,
    )
    nll, ppl, acceptance = pl.pallas_call(
        split_kernel,
        name="split",
        out_shape=(
            jax.ShapeDtypeStruct((1, ROWS), F32),
            jax.ShapeDtypeStruct((1, DOCS), F32),
            jax.ShapeDtypeStruct((1, DOCS), F32),
        ),
        in_specs=[vmem],
        out_specs=(vmem, vmem, vmem),
    )(final)
    return (nll, ppl.reshape(DOCS), acceptance.reshape(DOCS))


def solution(mesh):
    split = Mesh(mesh.devices.reshape(2, 8, 2, 2, 8), ("xh", "y", "c", "xl", "z"))
    rows = ("xh", "y", "c")
    parts = ("xl", "z")
    placed = (
        P(parts, rows, None),
        P(parts, rows, None),
        P(parts, rows, None),
        P(parts, rows, None),
        P(parts, rows),
        P(),
        P(),
        P(),
        P(),
        P(None, parts),
    )
    return jax.shard_map(
        shards, mesh=split, in_specs=placed, out_specs=(P(parts, rows), P(), P()), check_vma=False
    )
```

```python
import math

import jax
import jax.numpy as jnp
import numpy as np
from jax import lax
from jax.experimental import pallas as pl
from jax.experimental.pallas import tpu as pltpu
from jax.sharding import Mesh
from jax.sharding import PartitionSpec as P

HEADS = 12
HEAD_DIM = 64
ROT = 16
D = 768
ROWS = 128
SHARE = 1664
WIDE = 2 * SHARE
TILE = 256
TILES = WIDE // TILE
DOCS = 16
SEQ = 32
HALF = 256
SPAN = 512
NEGATIVE = -1e30
ROTARY_BASE = 10000.0
NORM_EPSILON = 1e-05
SPREAD_EPSILON = 0.0001
LOG2E = 1.4426950408889634
MESH = pl.DeviceIdType.MESH
F32 = jnp.float32
BF16 = jnp.bfloat16


def lanes(shape):
    return lax.broadcasted_iota(jnp.int32, shape, len(shape) - 1)


def rows_of(shape):
    return lax.broadcasted_iota(jnp.int32, shape, len(shape) - 2)


def rcopy(src, dst, ss, rs, **where):
    return pltpu.make_async_remote_copy(
        src_ref=src,
        dst_ref=dst,
        send_sem=ss,
        recv_sem=rs,
        device_id=where,
        device_id_type=MESH,
    )


def kernel(
    base_in,
    step_in,
    lengths_in,
    rank_in,
    q_in,
    k_in,
    v_in,
    hid_in,
    tgt_ref,
    gain_in,
    ow_in,
    un_ref,
    final_ref,
    base_ref,
    step_ref,
    lengths_ref,
    rank_ref,
    q_ref,
    k_ref,
    v_ref,
    hid_ref,
    gain_ref,
    ow_ref,
    packed,
    got,
    outs,
    att,
    qt,
    vt,
    s_scr,
    mx_ref,
    sum_ref,
    pv_ref,
    v_sum,
    v_pick,
    wide,
    rows_buf,
    relay,
    logit,
    tgts,
    stat_out,
    stats,
    seqs,
    a_send,
    a_recv,
    f_send,
    f_recv,
    r_send,
    r_recv,
    w_sem,
    c_send,
    c_recv,
    t_send,
    t_recv,
    s_send,
    s_recv,
    q_send,
    q_recv,
    i_sem,
    tie_buf,
    tie_sem,
):
    xh = lax.axis_index("xh")
    y = lax.axis_index("y")
    c = lax.axis_index("c")
    xl = lax.axis_index("xl")
    z = lax.axis_index("z")
    me = xh * 8 + y
    seq = me * 2 + c
    doc = xl * 8 + z
    sig = 1 - 2 * lax.rem(z, 2)
    z_up = lax.rem(z + sig + 8, 8)
    z_dn = lax.rem(z - sig + 8, 8)
    z_pair = z + sig

    barrier = pltpu.get_barrier_semaphore()

    xh_at, c_at, xl_at = [xh, 1 - xh], [c, 1 - c], [xl, 1 - xl]
    y_at = [y] + [lax.rem(y + k, 8) for k in range(1, 8)]
    z_at = [z] + [lax.rem(z + k, 8) for k in range(1, 8)]
    far_first = (4, 3, 5, 2, 6, 1, 7, 0)
    seq_peers = [
        {"xh": xh_at[i], "y": y_at[j], "c": c_at[k]}
        for i in (1, 0)
        for j in far_first
        for k in (0, 1)
        if i or j or k
    ]
    doc_peers = [
        {"xl": xl_at[i], "z": z_at[j]} for j in far_first for i in (1, 0) if i or j
    ]
    for where in seq_peers + doc_peers:
        pl.semaphore_signal(barrier, inc=1, device_id=where, device_id_type=MESH)

    fetches = [
        pltpu.make_async_copy(src, dst, i_sem.at[n])
        for n, (src, dst) in enumerate(
            (
                (base_in.at[seq], base_ref),
                (step_in, step_ref),
                (k_in, k_ref),
                (q_in, q_ref),
                (v_in, v_ref),
                (hid_in, hid_ref),
                (ow_in, ow_ref),
                (gain_in, gain_ref),
                (lengths_in, lengths_ref),
                (rank_in, rank_ref),
                (tgt_ref, tgts.at[0]),
            )
        )
    ]
    for fetch in fetches:
        fetch.start()
    mine = pltpu.make_async_copy(un_ref, wide.at[:, pl.ds(0, SHARE)], w_sem.at[4])
    mine.start()

    lane = lanes((ROWS, ROWS))
    low = lane < HEAD_DIM
    first = lax.rem(lane, HEAD_DIM) < ROT // 2
    low_half = low[:HEAD_DIM]

    for fetch in fetches[:5]:
        fetch.wait()

    base_cos = base_ref[0:1]
    base_sin = base_ref[1:2]
    cosine = base_cos * step_ref[0] - base_sin * step_ref[1]
    sine = base_sin * step_ref[0] + base_cos * step_ref[1]
    sine = jnp.where(first, -sine, sine)

    def turn(block):
        partner = jnp.where(first, pltpu.roll(block, ROWS - 8, 1), pltpu.roll(block, 8, 1))
        return block * cosine + partner * sine

    for pair in range(HEADS // 2):
        at = slice(pair * ROWS, (pair + 1) * ROWS)
        tk = turn(k_ref[:, at].astype(F32))
        tq = turn(q_ref[:, at].astype(F32))
        tv = v_ref[:, at].astype(F32)
        rk = pltpu.roll(tk, HEAD_DIM, 1)
        rq = pltpu.roll(tq, HEAD_DIM, 1)
        rv = pltpu.roll(tv, HEAD_DIM, 1)
        packed[2 * pair, 0:ROWS] = jnp.where(low, tk, rv).astype(BF16)
        packed[2 * pair + 1, 0:ROWS] = jnp.where(low, rk, tv).astype(BF16)
        packed[2 * pair, ROWS : ROWS + HEAD_DIM] = jnp.where(
            low_half, tq[:HEAD_DIM], rq[HEAD_DIM:]
        ).astype(BF16)
        packed[2 * pair + 1, ROWS : ROWS + HEAD_DIM] = jnp.where(
            low_half, rq[:HEAD_DIM], tq[HEAD_DIM:]
        ).astype(BF16)

    pl.semaphore_wait(barrier, SEQ - 1 + DOCS - 1)

    swaps = []
    passes = []
    for n, (start_row, count) in enumerate(((0, 288), (288, 96))):
        some = pl.ds(pl.multiple_of(c * (D // 2) + start_row, 32), count)
        landing = wide.at[some, pl.ds(SHARE, SHARE)]
        swaps.append(
            rcopy(un_ref.at[some], landing, w_sem.at[n], w_sem.at[2 + n], z=z_pair)
        )
        passes.append(rcopy(landing, landing, w_sem.at[5 + n], w_sem.at[7 + n], c=1 - c))
    for swap in swaps:
        swap.start()

    is_head = jnp.logical_and(y != 3, y != 7)
    my_slot = y - jnp.where(y > 3, 1, 0)
    my_head = jnp.where(is_head, xh * 6 + my_slot, -1)

    start = lax.rem(my_head, 4)
    my_group = lax.div(me, 4)

    def head_copy(h):
        yi = lax.rem(h, 6)
        return rcopy(
            packed.at[h],
            got.at[c, me],
            a_send.at[0],
            a_recv.at[my_group],
            xh=h // 6,
            y=yi + jnp.where(yi > 2, 1, 0),
        )

    tie_y = lax.rem(y + 4, 8)
    has_tie = jnp.logical_and(tie_y != 3, tie_y != 7)
    tie_head = jnp.where(has_tie, xh * 6 + tie_y - jnp.where(tie_y > 3, 1, 0), -1)
    tie_from = xh * 8 + lax.rem(y + 3, 8)
    relays = jnp.logical_and(y != 4, y != 0)
    tie_send = rcopy(
        packed.at[jnp.maximum(tie_head, 0)],
        tie_buf,
        a_send.at[0],
        tie_sem.at[0],
        xh=xh,
        y=lax.rem(y + 5, 8),
    )
    tie_pass = rcopy(
        tie_buf,
        got.at[c, tie_from],
        tie_sem.at[1],
        a_recv.at[lax.div(tie_from, 4)],
        xh=xh,
        y=lax.rem(y + 7, 8),
    )

    @pl.when(has_tie)
    def _():
        tie_send.start()

    def send_head(n, carry):
        h = 4 * lax.rem(n + me, 3) + lax.rem(my_group + 4 - n // 3, 4)

        @pl.when(jnp.logical_and(h != my_head, h != tie_head))
        def _():
            head_copy(h).start()

        @pl.when(h == my_head)
        def _():
            got[c, me] = packed[h]

        return carry

    lax.fori_loop(0, HEADS, send_head, 0)

    def target_copy(n):
        side = lax.rem(n, 2)
        step = n // 2
        move = jnp.where(
            step == 0, 0, jnp.where(step == 1, -sig, jnp.where(step == 2, 2 * sig, -3 * sig))
        )
        return rcopy(
            tgt_ref,
            tgts.at[n],
            t_send.at[0],
            t_recv.at[0],
            xl=lax.rem(xl + side, 2),
            z=lax.rem(z + move + 8, 8),
        )

    def send_target(n, carry):
        target_copy(n).start()
        return carry

    lax.fori_loop(1, 8, send_target, 0)

    @pl.when(relays)
    def _():
        tie_send.wait_recv()
        tie_pass.start()

    def arrival(g):
        def wait(count):
            part = got.at[c, pl.ds(4 * g, count)]
            rcopy(part, part, a_send.at[0], a_recv.at[g], xh=xh, y=y).wait_recv()

        @pl.when(g != my_group)
        def _():
            wait(4)

        @pl.when(g == my_group)
        def _():
            wait(3)

    def forward(g):
        part = got.at[c, pl.ds(4 * g, 4), pl.ds(0, ROWS)]
        return rcopy(part, part, f_send.at[g], f_recv.at[g], c=1 - c)

    def forwarded(g):
        part = got.at[1 - c, pl.ds(4 * g, 4), pl.ds(0, ROWS)]
        return rcopy(part, part, f_send.at[g], f_recv.at[g], c=1 - c)

    scale = LOG2E / math.sqrt(HEAD_DIM)

    def result_copy(i):
        return rcopy(
            outs.at[i],
            att.at[my_head],
            r_send.at[0],
            r_recv.at[0],
            xh=i // 8,
            y=lax.rem(i, 8),
        )

    def pair_of(gq, gk, diagonal):
        counts = [2, 4] if diagonal else [4, 4]

        def score(hq, b):
            uh, par = b // 2, b % 2
            keys = got[par, pl.ds(4 * gk + 2 * uh, 2), 0:ROWS, :].reshape(HALF, ROWS)
            s = lax.dot_general(
                keys,
                qt[gq, hq * HALF : (hq + 1) * HALF],
                (((1,), (1,)), ((), ())),
                preferred_element_type=F32,
            )
            if diagonal and uh == hq:
                row = rows_of((HALF, HALF))
                col = lanes((HALF, HALF))
                key = row + jnp.where(row >= ROWS, ROWS, 0) + par * ROWS
                query = col + jnp.where(col >= ROWS, ROWS, 0) + c * ROWS
                s = jnp.where(key <= query, s, NEGATIVE)
            s_scr[hq, b] = s
            return jnp.max(s.reshape(HALF // 8, 8, HALF), axis=0)

        def raise_top(hq, top):
            old = mx_ref[gq, hq]
            new = jnp.maximum(old, jnp.max(top, axis=0, keepdims=True) * scale)
            mx_ref[gq, hq] = new
            return new, jnp.exp2(old - new)

        def weigh(hq, b, new):
            p = jnp.exp2(s_scr[hq, b] * scale - new)
            return p.astype(BF16), jnp.sum(p.reshape(HALF // 8, 8, HALF), axis=0)

        def close(hq, parts, total, factor):
            sum_ref[gq, hq] = sum_ref[gq, hq] * factor + total
            pv_ref[gq, hq] = pv_ref[gq, hq] * factor + jnp.dot(
                vt[gk, :, 0 : len(parts) * HALF],
                jnp.concatenate(parts, axis=0),
                preferred_element_type=F32,
            )

        top = score(0, 0)
        for b in range(1, counts[0]):
            top = jnp.maximum(top, score(0, b))
        new, factor = raise_top(0, top)
        parts, total, top = [], 0.0, None
        for b in range(4):
            part = score(1, b)
            top = part if top is None else jnp.maximum(top, part)
            if b < counts[0]:
                p, add = weigh(0, b, new)
                parts.append(p)
                total = total + add
        close(0, parts, total, factor)
        new, factor = raise_top(1, top)
        parts, total = [], 0.0
        for b in range(counts[1]):
            p, add = weigh(1, b, new)
            parts.append(p)
            total = total + add
        close(1, parts, total, factor)

    def finish(gq):
        for hq in range(2):
            out = pv_ref[gq, hq] / jnp.sum(sum_ref[gq, hq], axis=0, keepdims=True)
            for u in range(2):
                i = 4 * gq + 2 * hq + u
                whole = out[:, u * ROWS : (u + 1) * ROWS].astype(BF16)
                outs[i] = whole

                @pl.when(i != me)
                def _():
                    result_copy(i).start()

                @pl.when(i == me)
                def _():
                    att[my_head] = whole

    def phase(p, carry):
        g = lax.rem(start + p, 4)
        for u in range(4):
            qp = got[c, 4 * g + u, ROWS : ROWS + HEAD_DIM].astype(F32)
            qt[g, u * ROWS : u * ROWS + HEAD_DIM] = jnp.where(low_half, qp, 0.0).astype(BF16)
            qt[g, u * ROWS + HEAD_DIM : (u + 1) * ROWS] = jnp.where(
                low_half, pltpu.roll(qp, HEAD_DIM, 1), 0.0
            ).astype(BF16)
        mx_ref[g] = jnp.full((2, 1, HALF), NEGATIVE, F32)
        sum_ref[g] = jnp.zeros((2, 8, HALF), F32)
        pv_ref[g] = jnp.zeros((2, HEAD_DIM, HALF), F32)
        forwarded(g).wait_recv()
        for uh in range(2):
            for par in range(2):
                block = got[par, pl.ds(4 * g + 2 * uh, 2), 0:ROWS, :].reshape(HALF, ROWS)
                turned = jnp.transpose(block.astype(F32))[HEAD_DIM:]
                at = (2 * uh + par) * HALF
                vt[g, :, at : at + HALF] = turned.astype(BF16)

        def visit(m, inner):
            other = lax.rem(start + m, 4)
            gq = jnp.maximum(g, other)
            gk = jnp.minimum(g, other)

            @pl.when(m < p)
            def _():
                pair_of(gq, gk, False)

            @pl.when(m == p)
            def _():
                pair_of(g, g, True)

            ready = jnp.where(gq < start, gq + 4 - start, jnp.where(start == 0, gq, 3))

            @pl.when(jnp.logical_and(p == ready, jnp.logical_or(m == p, gq != g)))
            def _():
                finish(gq)

            @pl.when(jnp.logical_and(m == 0, p < 3))
            def _():
                ahead = lax.rem(start + p + 1, 4)
                arrival(ahead)
                forward(ahead).start()

            return inner

        lax.fori_loop(0, p + 1, visit, 0)
        return carry

    @pl.when(is_head)
    def _():
        arrival(start)
        forward(start).start()
        lax.fori_loop(0, 4, phase, 0)

    for swap, pass_on in zip(swaps, passes):
        swap.wait_recv()
        pass_on.start()

    @pl.when(is_head)
    def _():
        part = att.at[pl.ds(0, HEADS - 1)]
        rcopy(part, part, r_send.at[0], r_recv.at[0], xh=xh, y=y).wait_recv()

    @pl.when(jnp.logical_not(is_head))
    def _():
        rcopy(att, att, r_send.at[0], r_recv.at[0], xh=xh, y=y).wait_recv()

    for fetch in fetches[5:]:
        fetch.wait()
    residual = hid_ref[...].astype(F32) + lax.dot_general(
        att[...].reshape(D, ROWS),
        ow_ref[...],
        (((0,), (0,)), ((), ())),
        preferred_element_type=F32,
    )
    center = residual - jnp.sum(residual, axis=1, keepdims=True) * (1.0 / D)
    spread = jnp.sum(center * center, axis=1, keepdims=True) * (1.0 / D)
    rows_buf[0] = (center * lax.rsqrt(spread + NORM_EPSILON) * gain_ref[...].reshape(1, D)).astype(BF16)

    def part_of(slot, h):
        if slot >= 8:
            return relay.at[slot - 8, pl.ds(h * HEAD_DIM, HEAD_DIM)]
        return rows_buf.at[slot, pl.ds(h * HEAD_DIM, HEAD_DIM)]

    def row_copy(n, h):
        where = {"z": z_dn}
        if n < 4:
            source, target = 2 * n, 2 * n + 1
            where = {"xl": 1 - xl}
        elif n == 4:
            source, target = 0, 2
        elif n == 5:
            source, target = 0, 8
            where = {"z": z_up}
        elif n == 6:
            source, target = 2, 9
            where = {"z": z_up}
        elif n == 7:
            source, target = 8, 4
        else:
            source, target = 9, 6
        return rcopy(
            part_of(source, h),
            part_of(target, h),
            c_send.at[2 * n + h],
            c_recv.at[2 * target + h],
            **where,
        )

    def row_wait(slot, h):
        part = part_of(slot, h)
        rcopy(part, part, c_send.at[0], c_recv.at[2 * slot + h], z=z_dn).wait_recv()

    for h in range(2):
        row_copy(4, h).start()
        row_copy(5, h).start()
        row_copy(0, h).start()
    mine.wait()
    for pass_on in passes:
        pass_on.wait_recv()

    part = tgts.at[pl.ds(1, 7)]
    rcopy(part, part, t_send.at[0], t_recv.at[0], z=z_dn).wait_recv()
    diagonal = lane == rows_of((ROWS, ROWS))
    other = xl * 8 + z_pair

    slot_j = (xl * 4 + z // 2) * 8

    def as_row(column):
        return jnp.sum(jnp.where(diagonal, column, 0.0), axis=0, keepdims=True)

    def score_rows(n, carry):
        @pl.when(n == 1)
        def _():
            for h in range(2):
                row_wait(8, h)
                row_copy(7, h).start()
                row_wait(2, h)
                row_copy(6, h).start()
                row_copy(1, h).start()
            for h in range(2):
                row_wait(1, h)

        @pl.when(n == 2)
        def _():
            row_wait(9, 0)
            row_copy(8, 0).start()
            row_wait(4, 0)
            row_copy(2, 0).start()

        @pl.when(n == 3)
        def _():
            row_wait(9, 1)
            row_copy(8, 1).start()
            row_wait(4, 1)
            row_copy(2, 1).start()
            for h in range(2):
                row_wait(3, h)

        @pl.when(n == 4)
        def _():
            row_wait(6, 0)
            row_copy(3, 0).start()

        @pl.when(n == 5)
        def _():
            row_wait(6, 1)
            row_copy(3, 1).start()
            for h in range(2):
                row_wait(5, h)

        @pl.when(n == 7)
        def _():
            for h in range(2):
                row_wait(7, h)

        block = rows_buf[n]
        top = jnp.full((ROWS, ROWS), NEGATIVE, F32)
        for k in range(TILES):
            s = jnp.dot(
                block, wide[:, k * TILE : (k + 1) * TILE], preferred_element_type=F32
            )
            logit[k] = s
            top = jnp.maximum(top, jnp.maximum(s[:, :ROWS], s[:, ROWS:]))

        wanted = jnp.broadcast_to(tgts[n], (ROWS, ROWS))
        wanted = jnp.sum(
            jnp.where(diagonal, wanted.astype(F32), 0.0), axis=1, keepdims=True
        ).astype(jnp.int32)
        here = wanted - doc * SHARE
        there = wanted - other * SHARE
        place = jnp.where(
            jnp.logical_and(here >= 0, here < SHARE),
            here,
            jnp.where(jnp.logical_and(there >= 0, there < SHARE), there + SHARE, -1),
        )
        place = jnp.broadcast_to(place, (ROWS, ROWS)) - lane
        top = jnp.max(top, axis=1, keepdims=True)
        top2 = jnp.broadcast_to(top * LOG2E, (ROWS, ROWS))
        v_sum[...] = jnp.zeros((ROWS, ROWS), F32)
        v_pick[...] = jnp.zeros((ROWS, ROWS), F32)

        def add_up(k, inner):
            total = v_sum[...]
            pick = v_pick[...]
            for g in range(TILE // ROWS):
                s = logit[k, :, g * ROWS : (g + 1) * ROWS]
                total = total + jnp.exp2(s * LOG2E - top2)
                pick = pick + jnp.where(place == k * TILE + g * ROWS, s, 0.0)
            v_sum[...] = total
            v_pick[...] = pick
            return inner

        lax.fori_loop(0, TILES, add_up, 0)
        lse = top + jnp.log(jnp.sum(v_sum[...], axis=1, keepdims=True))
        pick = jnp.sum(v_pick[...], axis=1, keepdims=True)
        stat_out[n] = jnp.where(rows_of((2, ROWS)) == 0, as_row(lse), as_row(pick))
        spot = slot_j + lax.rem(z - sig * lax.div(n, 2) + 8, 8)
        plane = lax.rem(xl + n, 2)
        stats[spot, plane] = stat_out[n]
        for where in doc_peers:
            rcopy(
                stat_out.at[n], stats.at[spot, plane], s_send.at[0], s_recv.at[0], **where
            ).start()

        return carry

    lax.fori_loop(0, 8, score_rows, 0)

    sent = stats.at[pl.ds(0, 60)]
    rcopy(sent, sent, s_send.at[0], s_recv.at[0], z=z_dn).wait_recv()
    entries = stats[...].reshape(8, DOCS, 2, ROWS)
    top = jnp.max(entries, axis=0)
    total = jnp.sum(jnp.exp(entries - top[None]), axis=0)
    pick = jnp.sum(entries, axis=0)
    shape = (DOCS, ROWS)
    row = rows_of(shape)
    col = lanes(shape)
    scored = jnp.where(
        rows_of((DOCS, 2, ROWS)) == 0, top + jnp.log(total), -pick
    )
    scored = jnp.sum(scored, axis=1)
    limit = jnp.zeros(shape, jnp.int32)
    for d in range(DOCS):
        limit = jnp.where(row == d, lengths_ref[(d % 2) * 8 + d // 2], limit)
    scored = jnp.where(seq * ROWS + col < limit, scored, 0.0)
    nll = jnp.sum(jnp.where(row == 2 * z + xl, scored, 0.0), axis=0, keepdims=True)
    doc_of = lax.rem(row, 2) * 8 + lax.div(row, 2)
    sums = jnp.sum(scored, axis=1, keepdims=True)
    seqs[seq] = jnp.sum(jnp.where(col == doc_of, sums, 0.0), axis=0, keepdims=True)

    for where in seq_peers:
        rcopy(seqs.at[seq], seqs.at[seq], q_send.at[0], q_recv.at[0], **where).start()

    @pl.when(is_head)
    def _():
        part = packed.at[pl.ds(0, HEADS - 1)]
        rcopy(part, part, a_send.at[0], a_recv.at[0], xh=xh, y=y).wait_send()
        part = outs.at[pl.ds(0, 15)]
        rcopy(part, part, r_send.at[0], r_recv.at[0], xh=xh, y=y).wait_send()
        for g in range(4):
            forward(g).wait_send()

    @pl.when(jnp.logical_not(is_head))
    def _():
        rcopy(packed, packed, a_send.at[0], a_recv.at[0], xh=xh, y=y).wait_send()

    @pl.when(relays)
    def _():
        tie_pass.wait_send()

    for copy in swaps + passes:
        copy.wait_send()
    for n in range(9):
        for h in range(2):
            row_copy(n, h).wait_send()
    part = tgts.at[pl.ds(1, 7)]
    rcopy(part, part, t_send.at[0], t_recv.at[0], z=z_dn).wait_send()
    rcopy(sent, sent, s_send.at[0], s_recv.at[0], z=z_dn).wait_send()
    others = seqs.at[pl.ds(0, SEQ - 1)]
    rcopy(others, others, q_send.at[0], q_recv.at[0], z=z_dn).wait_recv()
    line = jnp.sum(seqs[...], axis=0)
    valid = lanes((1, ROWS)) < DOCS
    count = jnp.ones((1, ROWS), F32)
    for d in range(DOCS):
        count = jnp.where(lanes((1, ROWS)) == d, lengths_ref[d].astype(F32), count)
    line = line / count
    column = jnp.sum(jnp.where(row == col, line, 0.0), axis=1, keepdims=True)
    mean = jnp.sum(line, axis=1, keepdims=True) * (1.0 / DOCS)
    off = jnp.where(valid, line - mean, 0.0)
    spread = jnp.sqrt(jnp.sum(off * off, axis=1, keepdims=True) * (1.0 / DOCS) + SPREAD_EPSILON)
    ahead = jnp.logical_or(
        column < line, jnp.logical_and(column == line, row < col)
    )
    rank = jnp.sum(jnp.where(ahead, 1.0, 0.0), axis=0, keepdims=True)
    scaled = rank_ref[0, 0] * (DOCS - 1)
    low_index = lax.div(scaled, 99)
    high_index = jnp.minimum(low_index + 1, DOCS - 1)
    fraction = (scaled - 99 * low_index).astype(F32) / 99.0
    hit_low = jnp.logical_and(valid, rank == low_index.astype(F32))
    hit_high = jnp.logical_and(valid, rank == high_index.astype(F32))
    low_value = jnp.sum(jnp.where(hit_low, line, 0.0), axis=1, keepdims=True)
    high_value = jnp.sum(jnp.where(hit_high, line, 0.0), axis=1, keepdims=True)
    level = (1.0 - fraction) * low_value + fraction * high_value
    accepted = jax.nn.sigmoid((level - line) / spread)
    row = rows_of((8, ROWS))
    final_ref[...] = jnp.where(row == 0, nll, jnp.where(row == 1, line, accepted))
    rcopy(others, others, q_send.at[0], q_recv.at[0], z=z_dn).wait_send()


def split_kernel(final_ref, nll_ref, ppl_ref, acc_ref):
    nll_ref[...] = final_ref[0:1]
    ppl_ref[...] = final_ref[1:2, :DOCS]
    acc_ref[...] = final_ref[2:3, :DOCS]


def turn_tables():
    spot = np.arange(ROWS) % HEAD_DIM
    freq = ROTARY_BASE ** (-2.0 * (spot % (ROT // 2)) / ROT)
    freq = np.where(spot < ROT, freq, 0.0)
    base = np.arange(SEQ)[:, None] * float(ROWS) * freq[None, :]
    step = np.arange(ROWS)[:, None] * freq[None, :]
    base = np.stack([np.cos(base), np.sin(base)], axis=1).astype(np.float32)
    step = np.stack([np.cos(step), np.sin(step)], axis=0).astype(np.float32)
    return base, step


def shards(
    hidden,
    queries,
    key_states,
    values,
    targets,
    lengths,
    keep_rank,
    out_weight,
    final_gain,
    unembed,
):
    base, step = turn_tables()
    vmem = pl.BlockSpec(memory_space=pltpu.VMEM)
    dma = pltpu.SemaphoreType.DMA
    final = pl.pallas_call(
        kernel,
        name="scoring",
        out_shape=jax.ShapeDtypeStruct((8, ROWS), F32),
        in_specs=[pl.BlockSpec(memory_space=pltpu.HBM)] * 12,
        out_specs=vmem,
        scratch_shapes=[
            pltpu.VMEM((2, ROWS), F32),
            pltpu.VMEM((2, ROWS, ROWS), F32),
            pltpu.SMEM((DOCS,), jnp.int32),
            pltpu.SMEM((1, 1), jnp.int32),
            pltpu.VMEM((ROWS, D), BF16),
            pltpu.VMEM((ROWS, D), BF16),
            pltpu.VMEM((ROWS, D), BF16),
            pltpu.VMEM((ROWS, D), BF16),
            pltpu.VMEM((D,), F32),
            pltpu.VMEM((D, D), BF16),
            pltpu.VMEM((HEADS, ROWS + HEAD_DIM, ROWS), BF16),
            pltpu.VMEM((2, 16, ROWS + HEAD_DIM, ROWS), BF16),
            pltpu.VMEM((16, HEAD_DIM, ROWS), BF16),
            pltpu.VMEM((HEADS, HEAD_DIM, ROWS), BF16),
            pltpu.VMEM((4, SPAN, ROWS), BF16),
            pltpu.VMEM((4, HEAD_DIM, 4 * HALF), BF16),
            pltpu.VMEM((2, 4, HALF, HALF), F32),
            pltpu.VMEM((4, 2, 1, HALF), F32),
            pltpu.VMEM((4, 2, 8, HALF), F32),
            pltpu.VMEM((4, 2, HEAD_DIM, HALF), F32),
            pltpu.VMEM((ROWS, ROWS), F32),
            pltpu.VMEM((ROWS, ROWS), F32),
            pltpu.VMEM((D, WIDE), BF16),
            pltpu.VMEM((8, ROWS, D), BF16),
            pltpu.VMEM((2, ROWS, D), BF16),
            pltpu.VMEM((TILES, ROWS, TILE), F32),
            pltpu.VMEM((8, 1, ROWS), jnp.int32),
            pltpu.VMEM((8, 2, ROWS), F32),
            pltpu.VMEM((64, 2, 2, ROWS), F32),
            pltpu.VMEM((SEQ, 1, ROWS), F32),
            dma((1,)),
            dma((4,)),
            dma((4,)),
            dma((4,)),
            dma((1,)),
            dma((1,)),
            dma((9,)),
            dma((18,)),
            dma((20,)),
            dma((1,)),
            dma((1,)),
            dma((1,)),
            dma((1,)),
            dma((1,)),
            dma((1,)),
            dma((11,)),
            pltpu.VMEM((ROWS + HEAD_DIM, ROWS), BF16),
            dma((2,)),
        ],
        compiler_params=pltpu.CompilerParams(
            collective_id=0, has_side_effects=True, vmem_limit_bytes=67043328
        ),
    )(
        jnp.asarray(base),
        jnp.asarray(step),
        lengths,
        keep_rank.reshape(1, 1),
        queries[0],
        key_states[0],
        values[0],
        hidden[0],
        targets,
        final_gain,
        out_weight,
        unembed,
    )
    nll, ppl, acceptance = pl.pallas_call(
        split_kernel,
        name="split",
        out_shape=(
            jax.ShapeDtypeStruct((1, ROWS), F32),
            jax.ShapeDtypeStruct((1, DOCS), F32),
            jax.ShapeDtypeStruct((1, DOCS), F32),
        ),
        in_specs=[vmem],
        out_specs=(vmem, vmem, vmem),
    )(final)
    return (nll, ppl.reshape(DOCS), acceptance.reshape(DOCS))


def solution(mesh):
    split = Mesh(mesh.devices.reshape(2, 8, 2, 2, 8), ("xh", "y", "c", "xl", "z"))
    rows = ("xh", "y", "c")
    parts = ("xl", "z")
    placed = (
        P(parts, rows, None),
        P(parts, rows, None),
        P(parts, rows, None),
        P(parts, rows, None),
        P(parts, rows),
        P(),
        P(),
        P(),
        P(),
        P(None, parts),
    )
    return jax.shard_map(
        shards, mesh=split, in_specs=placed, out_specs=(P(parts, rows), P(), P()), check_vma=False
    )
```
